128 devices in a mesh: dp: 1, ep2: 2 (over core), ep: 64 (over z, y, x).
Axes of the slice: x: 4, y: 4, z: 4, core: 2. Of those that a mesh axis runs over, the one named last changes fastest.
Arguments:
- tokens: bfloat16 [16384, 2048], P(('dp', 'ep2', 'ep'))
- expert_idx: int32 [16384, 8], P(('dp', 'ep2', 'ep'))
- gates: float32 [16384, 8], P(('dp', 'ep2', 'ep'))
- w_gate: bfloat16 [128, 2048, 768], P(('ep2', 'ep'))
- w_up: bfloat16 [128, 2048, 768], P(('ep2', 'ep'))
- w_down: bfloat16 [128, 768, 2048], P(('ep2', 'ep'))
Outputs:
- output: bfloat16 [16384, 2048], P(('dp', 'ep2', 'ep'))
All inputs are finite; a program needn't handle non-finite values.
Results may differ from the reference program's by a relative error of at most 0.00119.
Values are sent between devices in bfloat16 or wider.
A program may use at most 1 GiB of HBM per device.

```python
import jax
import jax.numpy as jnp
from jax import lax

GROUP_DEVS = 128
TOKENS = 128
HIDDEN = 2048
EXPERT_FF = 768
EXPERTS = 128
TOP_K = 8

LOCAL_EXPERTS = EXPERTS // GROUP_DEVS
EXPERT_CAP = (TOKENS * TOP_K + EXPERTS - 1) // EXPERTS
TOTAL_ROWS = GROUP_DEVS * TOKENS
EXPERT_ROWS = GROUP_DEVS * EXPERT_CAP


def draw_routing(route_key):
    key_pick, key_first, key_rest, key_bias = jax.random.split(route_key, 4)
    expert_ids = jnp.arange(EXPERTS, dtype=jnp.int32)
    local_pick = jax.random.randint(key_pick, (GROUP_DEVS, GROUP_DEVS), 0, LOCAL_EXPERTS)
    picked = (expert_ids % LOCAL_EXPERTS)[None, :] == jnp.repeat(local_pick, LOCAL_EXPERTS, axis=1)
    first_score = jax.random.randint(key_first, (GROUP_DEVS, EXPERTS), 0, 1024) + 2048
    rest_score = jax.random.randint(key_rest, (GROUP_DEVS, EXPERTS), 0, 1024) + jax.random.randint(key_bias, (1, EXPERTS), 0, 512)
    score = jnp.where(picked, first_score, rest_score) * EXPERTS + expert_ids[None, :]
    sequence = jnp.argsort(-score, axis=1).astype(jnp.int32)
    positions = (jnp.arange(TOKENS)[:, None] * TOP_K + jnp.arange(TOP_K)[None, :]) % EXPERTS
    chosen = jnp.take(sequence, positions.reshape(-1), axis=1)
    return chosen.reshape(TOTAL_ROWS, TOP_K)


def setup_inputs(seed: int = 0, part: int = 0) -> dict:
    root_key = jax.random.key(seed)
    shared_key, local_root = jax.random.split(root_key)
    part_key = jax.random.fold_in(local_root, part)
    key_tok, key_route, key_gate = jax.random.split(part_key, 3)
    key_wg, key_wu, key_wd = jax.random.split(shared_key, 3)
    tokens = jax.random.normal(key_tok, (TOTAL_ROWS, HIDDEN), jnp.float32).astype(jnp.bfloat16)
    expert_idx = draw_routing(key_route)
    gate_logits = jax.random.normal(key_gate, (TOTAL_ROWS, TOP_K), jnp.float32)
    gates = 0.5 * TOP_K * jax.nn.softmax(gate_logits, axis=-1)
    w_gate = (jax.random.normal(key_wg, (EXPERTS, HIDDEN, EXPERT_FF), jnp.float32) * HIDDEN ** -0.5).astype(jnp.bfloat16)
    w_up = (jax.random.normal(key_wu, (EXPERTS, HIDDEN, EXPERT_FF), jnp.float32) * HIDDEN ** -0.5).astype(jnp.bfloat16)
    w_down = (jax.random.normal(key_wd, (EXPERTS, EXPERT_FF, HIDDEN), jnp.float32) * EXPERT_FF ** -0.5).astype(jnp.bfloat16)
    return {'tokens': tokens, 'expert_idx': expert_idx, 'gates': gates, 'w_gate': w_gate, 'w_up': w_up, 'w_down': w_down}


def expert_ffn(operands):
    rows_in, gate_w, up_w, down_w = operands
    act_gate = jnp.dot(rows_in, gate_w, preferred_element_type=jnp.float32)
    act_up = jnp.dot(rows_in, up_w, preferred_element_type=jnp.float32)
    inner_act = (jax.nn.silu(act_gate) * act_up).astype(jnp.bfloat16)
    return jnp.dot(inner_act, down_w, preferred_element_type=jnp.float32).astype(jnp.bfloat16)


def reference(tokens, expert_idx, gates, w_gate, w_up, w_down):
    flat_ids = expert_idx.reshape(-1)
    n_items = flat_ids.shape[0]
    sort_order = jnp.argsort(flat_ids, stable=True)
    sorted_ids = flat_ids[sort_order]
    counts = jnp.bincount(flat_ids, length=EXPERTS)
    starts = jnp.cumsum(counts) - counts
    rank_sorted = (jnp.arange(n_items) - starts[sorted_ids]).astype(jnp.int32)
    slot_rank = jnp.zeros((n_items,), jnp.int32).at[sort_order].set(rank_sorted)
    token_of = jnp.arange(n_items) // TOP_K
    expert_in = jnp.zeros((EXPERTS, EXPERT_ROWS, HIDDEN), tokens.dtype).at[flat_ids, slot_rank].set(tokens[token_of])
    expert_out = lax.map(expert_ffn, (expert_in, w_gate, w_up, w_down))
    routed = expert_out[flat_ids, slot_rank].reshape(TOTAL_ROWS, TOP_K, HIDDEN)
    mixed = jnp.sum(gates[:, :, None] * routed.astype(jnp.float32), axis=1)
    return (tokens.astype(jnp.float32) + mixed).astype(jnp.bfloat16)
```

```python
import functools

import jax
import jax.numpy as jnp
from jax import lax
from jax.experimental import pallas as pl
from jax.experimental.pallas import tpu as pltpu
from jax.sharding import PartitionSpec as P

MESH = pl.DeviceIdType.MESH
STEP = 37
BACK = 45


def pick(arr, i):
    return arr[:, i:i + 1]


def kernel(idx_ref, gates_ref, tok_ref, wg_hbm, wu_hbm, wd_hbm, out_ref,
           wg, wu, wd, sbuf, rbuf, ybuf, ret, rm_ref, gk_ref, acc, hbuf,
           wsem, ssem, rsem, s2sem, r2sem):
    c = lax.axis_index('ep2')
    e = lax.axis_index('ep')
    mx = e % 4
    my = (e // 4) % 4
    mz = e // 16
    bf = jnp.bfloat16
    f32 = jnp.float32

    cps = [pltpu.make_async_copy(wg_hbm, wg, wsem.at[0]), pltpu.make_async_copy(wu_hbm, wu, wsem.at[1]),
           pltpu.make_async_copy(wd_hbm, wd, wsem.at[2])]
    for q in cps:
        q.start()

    def target(i, sign):
        k = (i * STEP) % 128
        dx = k % 4
        dy = (k // 4) % 4
        dz = (k // 16) % 4
        dc = k // 64
        x = (mx + sign * dx + 4) % 4
        y = (my + sign * dy + 4) % 4
        z = (mz + sign * dz + 4) % 4
        return (0, (c + dc) % 2, z * 16 + y * 4 + x)

    bar = pltpu.get_barrier_semaphore()

    def sig(i, carry):
        pl.semaphore_signal(bar, inc=1, device_id=target(i, 1), device_id_type=MESH)
        return carry

    lax.fori_loop(1, 128, sig, 0)

    idx = idx_ref[...]
    rel = ((idx - mx) & 3) + (((idx >> 2) - my) & 3) * 4 + (((idx >> 4) - mz) & 3) * 16 + (((idx >> 6) - c) & 1) * 64
    pos = (rel * BACK) & 127
    lane = lax.broadcasted_iota(jnp.int32, (128, 128), 1)
    row = lax.broadcasted_iota(jnp.int32, (128, 128), 0)
    m = jnp.zeros((128, 128), f32)
    gk = jnp.zeros((128, 128), f32)
    for j in range(8):
        hit = pick(pos, j) == lane
        m = jnp.where(hit, 1.0, m)
        gk = jnp.where(hit, gates_ref[:, j:j + 1], gk)
    lower = jnp.where(lane < row, 1.0, 0.0).astype(bf)
    rank = jnp.dot(lower, m.astype(bf), preferred_element_type=f32)
    rm_ref[...] = jnp.where(m > 0.5, rank + 1.0, 0.0).astype(bf)
    hi = gk.astype(bf)
    r1 = gk - hi.astype(f32)
    mid = r1.astype(bf)
    lo = (r1 - mid.astype(f32)).astype(bf)
    gk_ref[0:128, :] = hi
    gk_ref[128:256, :] = mid
    gk_ref[256:384, :] = lo

    def spread(b, n):
        k = lax.broadcasted_iota(jnp.int32, (128, n), 0)
        s = lax.broadcasted_iota(jnp.int32, (128, n), 1)
        return jnp.where(k == b * (n // 8) + (s >> 3), 1.0, 0.0).astype(bf)

    def build(b, carry):
        ex = spread(b, 128)
        slot = lax.broadcasted_iota(jnp.int32, (128, 128), 1)
        r = jnp.dot(rm_ref[...], ex, preferred_element_type=f32)
        dt = jnp.where(r == ((slot & 7) + 1).astype(f32), 1.0, 0.0)
        d = jnp.swapaxes(dt, 0, 1).astype(bf)
        for t in range(4):
            rows = jnp.dot(d, tok_ref[:, t * 512:(t + 1) * 512], preferred_element_type=f32).astype(bf)
            sbuf[pl.ds(b * 16, 16), :, t * 512:(t + 1) * 512] = rows.reshape(16, 8, 512)
        return carry

    lax.fori_loop(0, 8, build, 0)
    rbuf[0] = sbuf[0]
    pl.semaphore_wait(bar, 127)

    def out_copy(i):
        return pltpu.make_async_remote_copy(sbuf.at[i], rbuf.at[i], ssem.at[i], rsem.at[i], device_id=target(i, 1), device_id_type=MESH)

    def back_copy(i):
        return pltpu.make_async_remote_copy(ybuf.at[i], ret.at[i], s2sem.at[i], r2sem.at[i], device_id=target(i, -1), device_id_type=MESH)

    def loop(lo_, hi_, fn):
        def body(i, carry):
            fn(i)
            return carry
        lax.fori_loop(lo_, hi_, body, 0)

    loop(1, 128, lambda i: out_copy(i).start())
    for q in cps:
        q.wait()

    for g in range(4):
        lo_i, hi_i = max(1, g * 32), g * 32 + 32
        loop(lo_i, hi_i, lambda i: out_copy(i).wait_recv())

        def up(f, carry):
            fs = pl.ds(pl.multiple_of(f * 256, 256), 256)
            x = rbuf[g * 32:(g + 1) * 32].reshape(256, 2048)
            a = jnp.dot(x, wg[:, fs], preferred_element_type=f32)
            b = jnp.dot(x, wu[:, fs], preferred_element_type=f32)
            hbuf[:, fs] = (a * jax.nn.sigmoid(a) * b).astype(bf)
            return carry

        lax.fori_loop(0, 3, up, 0)

        def down(n, carry):
            ns = pl.ds(pl.multiple_of(n * 512, 512), 512)
            y = jnp.dot(hbuf[...], wd[:, ns], preferred_element_type=f32).astype(bf)
            ybuf[g * 32:(g + 1) * 32, :, ns] = y.reshape(32, 8, 512)
            return carry

        lax.fori_loop(0, 4, down, 0)
        if g == 0:
            ret[0] = ybuf[0]
        loop(lo_i, hi_i, lambda i: back_copy(i).start())

    for g in range(4):
        lo_i, hi_i = max(1, g * 32), g * 32 + 32
        ex = spread(g, 256)
        slot = lax.broadcasted_iota(jnp.int32, (128, 256), 1)
        r = jnp.dot(rm_ref[...], ex, preferred_element_type=f32)
        on = jnp.where(r == ((slot & 7) + 1).astype(f32), 1.0, 0.0)
        gx = jnp.dot(gk_ref[...], ex, preferred_element_type=f32)
        gx = (gx * jnp.concatenate([on, on, on], axis=0)).astype(bf)
        loop(lo_i, hi_i, lambda i: back_copy(i).wait_recv())

        def mix(n, carry):
            ns = pl.ds(pl.multiple_of(n * 256, 256), 256)
            y = ret[g * 32:(g + 1) * 32, :, ns].reshape(256, 256)
            p = jnp.dot(gx, y, preferred_element_type=f32)
            p = p[0:128] + p[128:256] + p[256:384]
            base = tok_ref[:, ns].astype(f32) if g == 0 else acc[:, ns]
            if g == 3:
                out_ref[:, ns] = (base + p).astype(bf)
            else:
                acc[:, ns] = base + p
            return carry

        lax.fori_loop(0, 8, mix, 0)

    loop(1, 128, lambda i: out_copy(i).wait_send())
    loop(1, 128, lambda i: back_copy(i).wait_send())


def solution(mesh):
    row_spec = P(('dp', 'ep2', 'ep'), None)
    weight_spec = P(('ep2', 'ep'), None, None)

    def local_step(tokens, expert_idx, gates, w_gate, w_up, w_down):
        vm = pl.BlockSpec(memory_space=pltpu.VMEM)
        anyw = pl.BlockSpec(memory_space=pl.ANY)
        bf = jnp.bfloat16
        return pl.pallas_call(
            kernel,
            out_shape=jax.ShapeDtypeStruct((128, 2048), bf),
            in_specs=[vm, vm, vm, anyw, anyw, anyw],
            out_specs=vm,
            scratch_shapes=[
                pltpu.VMEM((2048, 768), bf), pltpu.VMEM((2048, 768), bf), pltpu.VMEM((768, 2048), bf),
                pltpu.VMEM((128, 8, 2048), bf), pltpu.VMEM((128, 8, 2048), bf),
                pltpu.VMEM((128, 8, 2048), bf), pltpu.VMEM((128, 8, 2048), bf),
                pltpu.VMEM((128, 128), bf), pltpu.VMEM((384, 128), bf),
                pltpu.VMEM((128, 2048), jnp.float32), pltpu.VMEM((256, 768), bf),
                pltpu.SemaphoreType.DMA((3,)),
                pltpu.SemaphoreType.DMA((128,)), pltpu.SemaphoreType.DMA((128,)),
                pltpu.SemaphoreType.DMA((128,)), pltpu.SemaphoreType.DMA((128,)),
            ],
            compiler_params=pltpu.CompilerParams(collective_id=0, has_side_effects=True, vmem_limit_bytes=60 * 1024 * 1024),
        )(expert_idx, gates, tokens, w_gate[0], w_up[0], w_down[0])

    return jax.shard_map(local_step, mesh=mesh, in_specs=(row_spec, row_spec, row_spec, weight_spec, weight_spec, weight_spec),
                         out_specs=row_spec, check_vma=False)
```

```python
import functools

import jax
import jax.numpy as jnp
from jax import lax
from jax.experimental import pallas as pl
from jax.experimental.pallas import tpu as pltpu
from jax.sharding import PartitionSpec as P

MESH = pl.DeviceIdType.MESH
CUT = 10


def dec(j):
    return j % 3 + 1, (j % 9) // 3 + 1, j // 9


def third(q, u, v):
    return (q - u - v + 8) % 3 + 1


def slot_codes():
    codes = [0] * 128
    for j in range(18):
        u, v, dc = dec(j)
        for q in range(3):
            off = [0, 0, 0]
            off[q], off[(q + 1) % 3], off[(q + 2) % 3] = u, v, third(q, u, v)
            codes[3 * j + q] = off[0] + 4 * off[1] + 16 * off[2] + 64 * dc
            off = [0, 0, 0]
            off[(q + 1) % 3], off[(q + 2) % 3] = u, v
            codes[54 + 3 * j + q] = off[0] + 4 * off[1] + 16 * off[2] + 64 * dc
    for k in range(6):
        for m in range(3):
            codes[108 + 3 * k + m] = (k % 3 + 1) * 4 ** m + 64 * (k // 3)
    codes[126] = 64
    assert sorted(codes) == list(range(128))
    return codes


def loop(lo, hi, fn):
    def body(i, carry):
        fn(i)
        return carry
    lax.fori_loop(lo, hi, body, 0)


def each(*fns):
    def body(j):
        for q in range(3):
            for fn in fns:
                fn(j, q)
    return body


class Exchange:
    def __init__(self, co, core, sign, src, dst, rel, ssem, fsem, asem, rsem):
        self.co, self.core, self.sign = co, core, sign
        self.src, self.dst, self.rel = src, dst, rel
        self.ssem, self.fsem, self.asem, self.rsem = ssem, fsem, asem, rsem

    def to(self, axis, off, dc):
        p = list(self.co)
        if axis is not None:
            p[axis] = (p[axis] + self.sign * off + 4) % 4
        return (0, (self.core + dc) % 2, p[2] * 16 + p[1] * 4 + p[0])

    def copy(self, a, b, s, r, target):
        return pltpu.make_async_remote_copy(a, b, s, r, device_id=target, device_id_type=MESH)

    def a1(self, j, q):
        u, v, dc = dec(j)
        s = 3 * j + q
        self.copy(self.src.at[s], self.rel.at[s], self.ssem, self.asem.at[j], self.to(q, u, 0)).start()

    def a2(self, j, q):
        u, v, dc = dec(j)
        s = 3 * j + q
        self.copy(self.rel.at[s], self.rel.at[54 + s], self.fsem, self.asem.at[18 + j], self.to((q + 1) % 3, v, 0)).start()

    def a3(self, j, q):
        u, v, dc = dec(j)
        s = 3 * j + q
        self.copy(self.rel.at[54 + s], self.dst.at[s], self.fsem, self.rsem.at[j // CUT], self.to((q + 2) % 3, third(q, u, v), dc)).start()

    def b1(self, j, q):
        u, v, dc = dec(j)
        s = 3 * j + q
        self.copy(self.src.at[54 + s], self.rel.at[108 + s], self.ssem, self.asem.at[36 + j], self.to((q + 1) % 3, u, 0)).start()

    def b2(self, j, q):
        u, v, dc = dec(j)
        s = 3 * j + q
        self.copy(self.rel.at[108 + s], self.dst.at[54 + s], self.fsem, self.rsem.at[2 + j // CUT], self.to((q + 2) % 3, v, dc)).start()

    def c1(self, k, q):
        s = 108 + 3 * k + q
        self.copy(self.src.at[s], self.dst.at[s], self.ssem, self.rsem.at[4], self.to(q, k % 3 + 1, k // 3)).start()

    def c0(self):
        self.copy(self.src.at[126], self.dst.at[126], self.ssem, self.rsem.at[4], self.to(None, 0, 1)).start()

    def wait(self, ref, sem):
        pltpu.make_async_remote_copy(ref, ref, self.ssem, sem, device_id=self.to(None, 0, 1), device_id_type=MESH).wait_recv()

    def wait_a1(self, j):
        self.wait(self.rel.at[pl.ds(3 * j, 3)], self.asem.at[j])

    def wait_a2(self, j):
        self.wait(self.rel.at[pl.ds(54 + 3 * j, 3)], self.asem.at[18 + j])

    def wait_b1(self, j):
        self.wait(self.rel.at[pl.ds(108 + 3 * j, 3)], self.asem.at[36 + j])

    def wait_group(self, g):
        lo, n = GROUPS[g]
        n = n - 1 if g == 4 else n
        self.wait(self.dst.at[pl.ds(lo, n)], self.rsem.at[g])

    def drain(self):
        self.wait(self.src.at[pl.ds(0, 127)], self.ssem)
        self.wait(self.rel, self.fsem)


GROUPS = ((0, 3 * CUT), (3 * CUT, 54 - 3 * CUT), (54, 3 * CUT), (54 + 3 * CUT, 54 - 3 * CUT), (108, 20))


def kernel(code_ref, idx_ref, gates_ref, tok_ref, wg_hbm, wu_hbm, wd_hbm, out_ref,
           wg, wu, wd, sbuf, rbuf, ybuf, ret, rel1, rel2, rm_ref, gk_ref, acc, hbuf,
           wsem, ssem, asem1, rsem1, asem2, rsem2):
    c = lax.axis_index('ep2')
    e = lax.axis_index('ep')
    mx, my, mz = e % 4, (e // 4) % 4, e // 16
    bf = jnp.bfloat16
    f32 = jnp.float32

    cps = [pltpu.make_async_copy(wg_hbm, wg, wsem.at[0]), pltpu.make_async_copy(wu_hbm, wu, wsem.at[1]),
           pltpu.make_async_copy(wd_hbm, wd, wsem.at[2])]
    for q in cps:
        q.start()
    go = Exchange((mx, my, mz), c, 1, sbuf, rbuf, rel1, ssem.at[0], ssem.at[1], asem1, rsem1)
    back = Exchange((mx, my, mz), c, -1, ybuf, ret, rel2, ssem.at[2], ssem.at[3], asem2, rsem2)

    bar = pltpu.get_barrier_semaphore()

    def sig(k):
        for axis in range(3):
            for dc in range(2):
                pl.semaphore_signal(bar, inc=1, device_id=go.to(axis, k, dc), device_id_type=MESH)

    loop(1, 4, sig)
    pl.semaphore_signal(bar, inc=1, device_id=go.to(None, 0, 1), device_id_type=MESH)

    idx = idx_ref[...]
    code = ((idx - mx) & 3) + (((idx >> 2) - my) & 3) * 4 + (((idx >> 4) - mz) & 3) * 16 + (((idx >> 6) - c) & 1) * 64
    want = code_ref[0:1, :]
    lane = lax.broadcasted_iota(jnp.int32, (128, 128), 1)
    row = lax.broadcasted_iota(jnp.int32, (128, 128), 0)
    m = jnp.zeros((128, 128), f32)
    gk = jnp.zeros((128, 128), f32)
    for j in range(8):
        hit = code[:, j:j + 1] == want
        m = jnp.where(hit, 1.0, m)
        gk = jnp.where(hit, gates_ref[:, j:j + 1], gk)
    lower = jnp.where(lane < row, 1.0, 0.0).astype(bf)
    rank = jnp.dot(lower, m.astype(bf), preferred_element_type=f32)
    rm_ref[...] = jnp.where(m > 0.5, rank + 1.0, 0.0).astype(bf)
    hi = gk.astype(bf)
    r1 = gk - hi.astype(f32)
    mid = r1.astype(bf)
    lo = (r1 - mid.astype(f32)).astype(bf)
    gk_ref[0:128, :] = hi
    gk_ref[128:256, :] = mid
    gk_ref[256:384, :] = lo

    def spread(first, n):
        k = lax.broadcasted_iota(jnp.int32, (128, n), 0)
        s = lax.broadcasted_iota(jnp.int32, (128, n), 1)
        return jnp.where(k == first + (s >> 3), 1.0, 0.0).astype(bf)

    def chosen(first, n, ex):
        slot = lax.broadcasted_iota(jnp.int32, (128, n), 1)
        r = jnp.dot(rm_ref[...], ex, preferred_element_type=f32)
        return jnp.where(r == ((slot & 7) + 1).astype(f32), 1.0, 0.0)

    def build(b):
        d = jnp.swapaxes(chosen(b * 16, 128, spread(b * 16, 128)), 0, 1).astype(bf)
        for t in range(4):
            rows = jnp.dot(d, tok_ref[:, t * 512:(t + 1) * 512], preferred_element_type=f32).astype(bf)
            sbuf[pl.ds(b * 16, 16), :, t * 512:(t + 1) * 512] = rows.reshape(16, 8, 512)

    loop(0, 8, build)
    rbuf[127] = sbuf[127]
    pl.semaphore_wait(bar, 19)

    def ffn(g):
        lo_s, n = GROUPS[g]
        rows = n * 8

        def up(f):
            fs = pl.ds(pl.multiple_of(f * 256, 256), 256)
            x = rbuf[lo_s:lo_s + n].reshape(rows, 2048)
            a = jnp.dot(x, wg[:, fs], preferred_element_type=f32)
            b = jnp.dot(x, wu[:, fs], preferred_element_type=f32)
            hbuf[0:rows, fs] = (a * jax.nn.sigmoid(a) * b).astype(bf)

        loop(0, 3, up)

        def down(t):
            ns = pl.ds(pl.multiple_of(t * 512, 512), 512)
            y = jnp.dot(hbuf[0:rows, :], wd[:, ns], preferred_element_type=f32).astype(bf)
            ybuf[lo_s:lo_s + n, :, ns] = y.reshape(n, 8, 512)

        loop(0, 4, down)

    def mix(g, first, last):
        lo_s, n = GROUPS[g]
        rows = n * 8
        ex = spread(lo_s, rows)
        on = chosen(lo_s, rows, ex)
        gx = jnp.dot(gk_ref[...], ex, preferred_element_type=f32)
        gx = (gx * jnp.concatenate([on, on, on], axis=0)).astype(bf)
        back.wait_group(g)

        def part(t):
            ns = pl.ds(pl.multiple_of(t * 256, 256), 256)
            y = ret[lo_s:lo_s + n, :, ns].reshape(rows, 256)
            p = jnp.dot(gx, y, preferred_element_type=f32)
            p = p[0:128] + p[128:256] + p[256:384]
            base = tok_ref[:, ns].astype(f32) if first else acc[:, ns]
            if last:
                out_ref[:, ns] = (base + p).astype(bf)
            else:
                acc[:, ns] = base + p

        loop(0, 8, part)

    def fwd(x, wait, move):
        def body(j):
            wait(j)
            for q in range(3):
                move(j, q)
        return body

    loop(0, 18, each(go.a1))

    def second(j):
        go.wait_a1(j)
        for q in range(3):
            go.a2(j, q)
            go.b1(j, q)

    loop(0, 18, second)
    go.c0()
    loop(0, 6, each(go.c1))

    def third_hop(j):
        go.wait_a2(j)
        for q in range(3):
            go.a3(j, q)
        go.wait_b1(j)
        for q in range(3):
            go.b2(j, q)

    loop(0, 18, third_hop)
    for q in cps:
        q.wait()

    go.wait_group(0)
    ffn(0)
    loop(0, CUT, each(back.a1))
    go.wait_group(1)
    ffn(1)
    loop(CUT, 18, each(back.a1))
    loop(0, CUT, fwd(back, back.wait_a1, back.a2))
    go.wait_group(2)
    ffn(2)
    loop(0, CUT, each(back.b1))
    loop(CUT, 18, fwd(back, back.wait_a1, back.a2))
    go.wait_group(3)
    ffn(3)
    loop(CUT, 18, each(back.b1))
    loop(0, CUT, fwd(back, back.wait_a2, back.a3))
    go.wait_group(4)
    ffn(4)
    ret[127] = ybuf[127]
    back.c0()
    loop(0, 6, each(back.c1))
    loop(CUT, 18, fwd(back, back.wait_a2, back.a3))
    loop(0, 18, fwd(back, back.wait_b1, back.b2))
    go.drain()
    mix(0, True, False)
    mix(1, False, False)
    mix(4, False, False)
    mix(2, False, False)
    mix(3, False, True)
    back.drain()


def solution(mesh):
    row_spec = P(('dp', 'ep2', 'ep'), None)
    weight_spec = P(('ep2', 'ep'), None, None)

    def local_step(tokens, expert_idx, gates, w_gate, w_up, w_down):
        vm = pl.BlockSpec(memory_space=pltpu.VMEM)
        anyw = pl.BlockSpec(memory_space=pl.ANY)
        bf = jnp.bfloat16
        codes = jnp.broadcast_to(jnp.array(slot_codes(), jnp.int32)[None, :], (8, 128))
        dma = pltpu.SemaphoreType.DMA
        return pl.pallas_call(
            kernel,
            out_shape=jax.ShapeDtypeStruct((128, 2048), bf),
            in_specs=[vm, vm, vm, vm, anyw, anyw, anyw],
            out_specs=vm,
            scratch_shapes=[
                pltpu.VMEM((2048, 768), bf), pltpu.VMEM((2048, 768), bf), pltpu.VMEM((768, 2048), bf),
                pltpu.VMEM((128, 8, 2048), bf), pltpu.VMEM((128, 8, 2048), bf),
                pltpu.VMEM((128, 8, 2048), bf), pltpu.VMEM((128, 8, 2048), bf),
                pltpu.VMEM((162, 8, 2048), bf), pltpu.VMEM((162, 8, 2048), bf),
                pltpu.VMEM((128, 128), bf), pltpu.VMEM((384, 128), bf),
                pltpu.VMEM((128, 2048), jnp.float32), pltpu.VMEM((256, 768), bf),
                dma((3,)), dma((4,)), dma((54,)), dma((5,)), dma((54,)), dma((5,)),
            ],
            compiler_params=pltpu.CompilerParams(collective_id=0, has_side_effects=True, vmem_limit_bytes=60 * 1024 * 1024),
        )(codes, expert_idx, gates, tokens, w_gate[0], w_up[0], w_down[0])

    return jax.shard_map(local_step, mesh=mesh, in_specs=(row_spec, row_spec, row_spec, weight_spec, weight_spec, weight_spec),
                         out_specs=row_spec, check_vma=False)
```

```python
import jax
import jax.numpy as jnp
import numpy as np
from jax import lax
from jax.experimental import pallas as pl
from jax.experimental.pallas import tpu as pltpu
from jax.sharding import PartitionSpec as P

MESH = pl.DeviceIdType.MESH
CUT = 8
D = 2048
TURNS = 18
T = 128
HALF = (2, 4, 4, 4)
AXES = range(3)
NEXT = (1, 3, 2)
COLS = ((0, 768), (768, 640), (1408, 640))
WEIGHT = (1, 4, 16)


def dec(j):
    return j % 3 + 1, (j % 9) // 3 + 1, j // 9


def third(q, u, v):
    return (q - u - v + 8) % 3 + 1


def offsets(kind, j, q):
    off = [0, 0, 0]
    if kind == 0:
        u, v, dc = dec(j)
        off[q], off[(q + 1) % 3], off[(q + 2) % 3] = u, v, third(q, u, v)
    elif kind == 1:
        u, v, dc = dec(j)
        off[(q + 1) % 3], off[(q + 2) % 3] = u, v
    else:
        off[q], dc = j % 3 + 1, j // 3
    return off, dc


def slot_codes():
    codes = [0] * 128
    for kind, n in ((0, TURNS), (1, TURNS), (2, 6)):
        for j in range(n):
            for q in AXES:
                off, dc = offsets(kind, j, q)
                codes[54 * kind + 3 * j + q] = off[0] + 4 * off[1] + 16 * off[2] + 64 * dc
    codes[126] = 64
    assert sorted(codes) == list(range(128))
    return codes


def loop(lo, hi, fn):
    def body(i, carry):
        fn(i)
        return carry
    lax.fori_loop(lo, hi, body, 0)


def each(*fns):
    def body(j):
        for q in AXES:
            for fn in fns:
                fn(j, q)
    return body


def target(co, core, axis, off, dc):
    p = list(co)
    if axis is not None:
        p[axis] = (p[axis] + off) % 4
    return (0, (core + dc) % 2, p[2] * 16 + p[1] * 4 + p[0])


def iota(dim, *shape):
    return lax.broadcasted_iota(jnp.int32, shape, dim)


def onehot(mask, dtype=jnp.bfloat16):
    return jnp.where(mask, 1.0, 0.0).astype(dtype)


class Exchange:
    def __init__(self, co, core, sign, src, dst, rel, ssem, fsem, asem, rsem):
        self.co, self.core, self.sign = co, core, sign
        self.src, self.dst, self.rel = src, dst, rel
        self.ssem, self.fsem, self.asem, self.rsem = ssem, fsem, asem, rsem

    def to(self, axis, off, dc):
        return target(self.co, self.core, axis, self.sign * off + 4, dc)

    def copy(self, a, b, s, r, dest):
        return pltpu.make_async_remote_copy(a, b, s, r, device_id=dest, device_id_type=MESH)

    def a1(self, j, q):
        u, v, dc = dec(j)
        s = 3 * j + q
        self.copy(self.src.at[s], self.rel.at[s], self.ssem, self.asem.at[j], self.to(q, u, 0)).start()

    def a2(self, j, q):
        u, v, dc = dec(j)
        s = 3 * j + q
        self.copy(self.rel.at[s], self.rel.at[54 + s], self.fsem, self.asem.at[TURNS + j], self.to((q + 1) % 3, v, 0)).start()

    def a3(self, j, q):
        u, v, dc = dec(j)
        s = 3 * j + q
        self.copy(self.rel.at[54 + s], self.dst.at[s], self.fsem, self.rsem.at[(j + 10 - CUT) // 10], self.to((q + 2) % 3, third(q, u, v), dc)).start()

    def b1(self, j, q):
        u, v, dc = dec(j)
        s = 3 * j + q
        self.copy(self.src.at[54 + s], self.rel.at[108 + s], self.ssem, self.asem.at[2 * TURNS + j], self.to((q + 1) % 3, u, 0)).start()

    def b2(self, j, q):
        u, v, dc = dec(j)
        s = 3 * j + q
        self.copy(self.rel.at[108 + s], self.dst.at[54 + s], self.fsem, self.rsem.at[2 + (j + 10 - CUT) // 10], self.to((q + 2) % 3, v, dc)).start()

    def c1(self, k, q):
        s = 108 + 3 * k + q
        self.copy(self.src.at[s], self.dst.at[s], self.ssem, self.rsem.at[4], self.to(q, k % 3 + 1, k // 3)).start()

    def c0(self):
        self.copy(self.src.at[126], self.dst.at[126], self.ssem, self.rsem.at[4], self.to(None, 0, 1)).start()

    def wait(self, ref, sem):
        pltpu.make_async_remote_copy(ref, ref, self.ssem, sem, device_id=self.to(None, 0, 1), device_id_type=MESH).wait_recv()

    def wait_a1(self, j):
        self.wait(self.rel.at[pl.ds(3 * j, 3)], self.asem.at[j])

    def wait_a2(self, j):
        self.wait(self.rel.at[pl.ds(54 + 3 * j, 3)], self.asem.at[TURNS + j])

    def wait_b1(self, j):
        self.wait(self.rel.at[pl.ds(108 + 3 * j, 3)], self.asem.at[2 * TURNS + j])

    def wait_group(self, g):
        lo, n = GROUPS[g]
        n = n - 1 if g == 4 else n
        self.wait(self.dst.at[pl.ds(lo, n)], self.rsem.at[g])

    def drain(self):
        self.wait(self.src.at[pl.ds(0, 127)], self.ssem)
        self.wait(self.rel, self.fsem)


EARLY, LATE = 3 * CUT, 54 - 3 * CUT
GROUPS = ((0, EARLY), (EARLY, LATE), (54, EARLY), (54 + EARLY, LATE), (108, 20))


def kernel(code_hbm, idx_hbm, gates_hbm, tok_hbm, wg_hbm, wu_hbm, wd_hbm, out_ref,
           code_ref, idx_ref, gates_ref, tok_ref, wg, wu, wd, toka, idxa, bld, mid, rbuf, xg, ybuf, ret, rel2, rm_ref, gk_ref, acc, hbuf,
           *rest):
    gx_refs = rest[:5]
    wsem, ssem, tsem, isem, bsem, csem, asem2, rsem2 = rest[5:]
    c = lax.axis_index('ep2')
    e = lax.axis_index('ep')
    me = (e % 4, (e // 4) % 4, e // 16)
    bf = jnp.bfloat16
    f32 = jnp.float32

    cps = [pltpu.make_async_copy(wg_hbm, wg, wsem.at[0]), pltpu.make_async_copy(wu_hbm, wu, wsem.at[1]),
           pltpu.make_async_copy(wd_hbm, wd, wsem.at[2])]
    small = [pltpu.make_async_copy(a, b, wsem.at[3 + i]) for i, (a, b) in enumerate(
        ((idx_hbm, idx_ref), (tok_hbm, tok_ref), (gates_hbm, gates_ref), (code_hbm, code_ref)))]
    back = Exchange(me, c, -1, ybuf, ret, rel2, ssem.at[4], ssem.at[5], asem2, rsem2)

    def to(axis, off, dc):
        return target(me, c, axis, off, dc)

    for q in small:
        q.start()
    bar = pltpu.get_barrier_semaphore()

    def sig(k):
        for axis in AXES:
            for dc in range(2):
                pl.semaphore_signal(bar, inc=1, device_id=to(axis, k, dc), device_id_type=MESH)

    loop(1, 4, sig)
    pl.semaphore_signal(bar, inc=1, device_id=to(None, 0, 1), device_id_type=MESH)
    before = onehot(iota(0, T, T) < iota(1, T, T))

    def ranked(idx8, want):
        m = jnp.zeros(want.shape, f32)
        for j in range(8):
            m = jnp.where(idx8[j:j + 1, :] == want, 1.0, m)
        rank = jnp.dot(m.astype(bf), before, preferred_element_type=f32)
        return jnp.where(m > 0.5, rank + 1.0, 0.0)

    def select(idx8, p):
        k = iota(0, 32, 128)
        b, d = (p + 1) % 3, (p + 2) % 3
        want = (((c + (k >> 4)) & 1) * 64 + me[p] * WEIGHT[p] + ((me[b] + (k >> 2)) & 3) * WEIGHT[b]
                + ((me[d] + k) & 3) * WEIGHT[d])
        rm = ranked(idx8, want).astype(bf)
        ex = onehot((iota(0, 256, 32) >> 3) == iota(1, 256, 32))
        r = jnp.dot(ex, rm, preferred_element_type=f32)
        return onehot(r == ((iota(0, 256, T) & 7) + 1).astype(f32))

    def cols(p):
        return pl.ds(COLS[p][0], COLS[p][1])

    def build(p, a):
        n = COLS[p][1]
        if a == 0:
            rows = jnp.dot(select(idx_ref[...], p), tok_ref[:, cols(p)], preferred_element_type=f32).astype(bf)
        else:
            rows = jnp.dot(select(idxa[p, a - 1], p), toka[a - 1, :, cols(p)], preferred_element_type=f32).astype(bf)
        rows = rows.reshape(2, 4, 4, 8, n)
        for dc in range(2):
            mid[dc, 0, a, :, :, cols(p)] = rows[dc, 0]
            for v in NEXT:
                bld[dc, v - 1, a, :, :, cols(p)] = rows[dc, v]

    def remote(a, b, s, r, dest):
        return pltpu.make_async_remote_copy(a, b, s, r, device_id=dest, device_id_type=MESH)

    def take(ref, sem):
        remote(ref, ref, ssem.at[0], sem, to(None, 0, 1)).wait_recv()

    def gather_tokens():
        for u in (1, 3, 2):
            for p in AXES:
                remote(idx_ref, idxa.at[p, u - 1], ssem.at[0], isem.at[p, u - 1], to(p, u, 0)).start()
                if u != 2:
                    remote(tok_ref.at[:, cols(p)], toka.at[u - 1, :, cols(p)], ssem.at[1], tsem.at[p, u - 1], to(p, u, 0)).start()

    def pass_on(p, a):
        lo_c, n = COLS[p]
        part = pl.ds(lo_c, 384) if a == 1 else pl.ds(lo_c + 384, n - 384)
        remote(toka.at[a - 1, :, part], toka.at[1, :, part], ssem.at[6], tsem.at[p, 1], to(p, a, 0)).start()

    def second(dc, a, p):
        for v in NEXT:
            remote(bld.at[dc, v - 1, a, :, :, cols(p)], mid.at[dc, v, a, :, :, cols(p)], ssem.at[2], bsem.at[dc, p, v - 1],
                   to((p + 1) % 3, v, 0)).start()

    def place(p, v, w, dc, ref):
        if p == 0:
            return ref.at[dc, w, v, :, :, cols(0)]
        if p == 1:
            return ref.at[dc, v, :, w, :, cols(1)]
        return ref.at[dc, :, w, v, :, cols(2)]

    def last(dc, v):
        for p in AXES:
            if v:
                take(mid.at[dc, v, :, :, :, cols(p)], bsem.at[dc, p, v - 1])
            for w in range(1 - dc, 4):
                remote(mid.at[dc, v, :, w, :, cols(p)], place(p, v, w, dc, rbuf), ssem.at[3 + 4 * dc], csem.at[dc, p],
                       to((p + 2) % 3, w, dc) if w else to(None, 0, 1)).start()
            if dc == 0:
                place(p, v, 0, 0, rbuf)[...] = mid[0, v, :, 0, :, cols(p)]

    for q in small:
        q.wait()
    for p in AXES:
        build(p, 0)
    pl.semaphore_wait(bar, 19)
    for q in cps:
        q.start()
    gather_tokens()
    for dc in range(2):
        for p in AXES:
            second(dc, 0, p)
    for a in (1, 3):
        for p in AXES:
            take(toka.at[a - 1, :, cols(p)], tsem.at[p, a - 1])
            pass_on(p, a)
    for a in NEXT:
        for p in AXES:
            take(idxa.at[p, a - 1], isem.at[p, a - 1])
            if a == 2:
                take(toka.at[a - 1, :, cols(p)], tsem.at[p, a - 1])
            build(p, a)
            second(0, a, p)
    last(0, 0)
    for a in (1, 3):
        for p in AXES:
            second(1, a, p)

    rel = (((idx_ref[...] >> 6) - c) & 1) << 6
    for d in AXES:
        rel += (((idx_ref[...] >> (2 * d)) - me[d]) & 3) << (2 * d)
    want = code_ref[...]
    rm_ref[...] = jnp.swapaxes(ranked(rel, want), 0, 1).astype(bf)
    gk = jnp.zeros((T, T), f32)
    for j in range(8):
        gk = jnp.where(rel[j:j + 1, :] == want, gates_ref[j:j + 1, :], gk)
    gk = jnp.swapaxes(gk, 0, 1)
    hi = gk.astype(bf)
    r1 = gk - hi.astype(f32)
    md = r1.astype(bf)
    lo = (r1 - md.astype(f32)).astype(bf)
    gk_ref[...] = jnp.concatenate([hi, md, lo], axis=0)

    def spread(first, n):
        return onehot(iota(0, T, n) == first + (iota(1, T, n) >> 3))

    def chosen(n, ex):
        r = jnp.dot(rm_ref[...], ex, preferred_element_type=f32)
        return onehot(r == ((iota(1, T, n) & 7) + 1).astype(f32), f32)

    for g in range(5):
        ex = spread(GROUPS[g][0], GROUPS[g][1] * 8)
        on = chosen(GROUPS[g][1] * 8, ex)
        gx = jnp.dot(gk_ref[...], ex, preferred_element_type=f32)
        gx_refs[g][...] = (gx * jnp.concatenate([on, on, on], axis=0)).astype(bf)


    for v in NEXT:
        last(0, v)
    for p in AXES:
        second(1, 2, p)
    for v in (0, *NEXT):
        last(1, v)
    for q in cps:
        q.wait()

    def fetch(kind, lo_j, hi_j):
        def body(j):
            for q in AXES:
                off, dc = offsets(kind, j, q)
                xg[3 * (j - lo_j) + q] = rbuf[dc, off[2], off[1], off[0]]
        loop(lo_j, hi_j, body)

    def arrived(dc):
        if dc == 0:
            take(rbuf.at[0, 1:4, :, :, :, cols(0)], csem.at[0, 0])
            take(rbuf.at[0, :, :, 1:4, :, cols(1)], csem.at[0, 1])
            take(rbuf.at[0, :, 1:4, :, :, cols(2)], csem.at[0, 2])
        else:
            for p in AXES:
                take(rbuf.at[1, :, :, :, :, cols(p)], csem.at[1, p])

    def ffn(g):
        lo_s, n = GROUPS[g]
        rows = n * 8

        def up(f):
            fs = pl.ds(pl.multiple_of(f * 256, 256), 256)
            x = xg[0:n].reshape(rows, 2048)
            a = jnp.dot(x, wg[:, fs], preferred_element_type=f32)
            b = jnp.dot(x, wu[:, fs], preferred_element_type=f32)
            hbuf[0:rows, fs] = (a * jax.nn.sigmoid(a) * b).astype(bf)

        loop(0, 3, up)

        def down(t):
            ns = pl.ds(pl.multiple_of(t * 512, 512), 512)
            y = jnp.dot(hbuf[0:rows, :], wd[:, ns], preferred_element_type=f32).astype(bf)
            ybuf[lo_s:lo_s + n, :, ns] = y.reshape(n, 8, 512)

        loop(0, 4, down)

    def mix(g, first, last):
        lo_s, n = GROUPS[g]
        rows = n * 8
        gx = gx_refs[g][...]
        back.wait_group(g)

        def part(t):
            ns = pl.ds(pl.multiple_of(t * 256, 256), 256)
            y = ret[lo_s:lo_s + n, :, ns].reshape(rows, 256)
            p = jnp.dot(gx, y, preferred_element_type=f32)
            p = p[:T] + p[T:2 * T] + p[2 * T:]
            base = tok_ref[:, ns].astype(f32) if first else acc[:, ns]
            if last:
                out_ref[:, ns] = (base + p).astype(bf)
            else:
                acc[:, ns] = base + p

        loop(0, 8, part)

    def fwd(x, wait, move):
        def body(j):
            wait(j)
            for q in AXES:
                move(j, q)
        return body

    arrived(0)
    fetch(0, 0, CUT)
    ffn(0)
    loop(0, CUT, each(back.a1))
    fetch(1, 0, CUT)
    ffn(2)
    loop(0, CUT, each(back.b1))
    arrived(1)
    fetch(0, CUT, TURNS)
    ffn(1)
    loop(CUT, TURNS, each(back.a1))
    loop(0, CUT, fwd(back, back.wait_a1, back.a2))
    fetch(1, CUT, TURNS)
    ffn(3)
    loop(CUT, TURNS, each(back.b1))
    loop(CUT, TURNS, fwd(back, back.wait_a1, back.a2))
    fetch(2, 0, 6)
    for dc in range(2):
        xg[19 - dc] = rbuf[dc, 0, 0, 0]
    ffn(4)
    ret[127] = ybuf[127]
    back.c0()
    loop(0, 6, each(back.c1))
    loop(0, CUT, fwd(back, back.wait_a2, back.a3))
    loop(0, CUT, fwd(back, back.wait_b1, back.b2))
    loop(CUT, TURNS, fwd(back, back.wait_a2, back.a3))
    loop(CUT, TURNS, fwd(back, back.wait_b1, back.b2))
    take(idxa, ssem.at[0])
    take(toka.at[0:2], ssem.at[1])
    take(toka.at[0], ssem.at[6])
    take(bld, ssem.at[2])
    take(mid.at[0, :, :, 1:4], ssem.at[3])
    take(mid.at[1], ssem.at[7])
    mix(4, True, False)
    mix(0, False, False)
    mix(2, False, False)
    mix(1, False, False)
    mix(3, False, True)
    back.drain()


def solution(mesh):
    row_spec = P(('dp', 'ep2', 'ep'), None)
    weight_spec = P(('ep2', 'ep'), None, None)

    def local_step(tokens, expert_idx, gates, w_gate, w_up, w_down):
        vm = pl.BlockSpec(memory_space=pltpu.VMEM)
        anyw = pl.BlockSpec(memory_space=pl.ANY)
        bf = jnp.bfloat16
        codes = jnp.array(np.repeat(np.array(slot_codes(), np.int32)[:, None], 128, axis=1))
        dma = pltpu.SemaphoreType.DMA

        def vmem(*shape):
            return pltpu.VMEM(shape, bf)

        def rows(*shape):
            return vmem(*shape, 8, D)

        return pl.pallas_call(
            kernel,
            out_shape=jax.ShapeDtypeStruct((128, D), bf),
            in_specs=[anyw] * 7,
            out_specs=vm,
            scratch_shapes=[
                pltpu.VMEM((T, T), jnp.int32), pltpu.VMEM((8, T), jnp.int32), pltpu.VMEM((8, T), jnp.float32), vmem(T, D),
                vmem(D, 768), vmem(D, 768), vmem(768, D),
                vmem(3, T, D), pltpu.VMEM((3, 3, 8, T), jnp.int32),
                rows(2, 3, 4, 4), rows(*HALF), rows(*HALF), rows(32), rows(T), rows(T), rows(9 * TURNS),
                vmem(T, T), vmem(3 * T, T), pltpu.VMEM((T, D), jnp.float32), vmem(256, 768),
                *[vmem(3 * T, n * 8) for _, n in GROUPS],
                *[dma(n) for n in ((7,), (8,), (3, 3), (3, 3), (2, 3, 3), (2, 3), (3 * TURNS,), (5,))],
            ],
            compiler_params=pltpu.CompilerParams(collective_id=0, has_side_effects=True, vmem_limit_bytes=60 << 20),
        )(codes, expert_idx.T, gates.T, tokens, w_gate[0], w_up[0], w_down[0])

    return jax.shard_map(local_step, mesh=mesh, in_specs=(row_spec, row_spec, row_spec, weight_spec, weight_spec, weight_spec),
                         out_specs=row_spec, check_vma=False)
```

```python
import jax
import jax.numpy as jnp
import numpy as np
from jax import lax
from jax.experimental import pallas as pl
from jax.experimental.pallas import tpu as pltpu
from jax.sharding import PartitionSpec as P

MESH = pl.DeviceIdType.MESH
CUT = 8
D = 2048
TURNS = 18
T = 128
HALF = (2, 4, 4, 4)
AXES = range(3)
NEXT = (1, 3, 2)
COLS = ((0, 768), (768, 640), (1408, 640))
WEIGHT = (1, 4, 16)


def dec(j):
    return j % 3 + 1, (j % 9) // 3 + 1, j // 9


def third(q, u, v):
    return (q - u - v + 8) % 3 + 1


def offsets(kind, j, q):
    off = [0, 0, 0]
    if kind == 0:
        u, v, dc = dec(j)
        off[q], off[(q + 1) % 3], off[(q + 2) % 3] = u, v, third(q, u, v)
    elif kind == 1:
        u, v, dc = dec(j)
        off[(q + 1) % 3], off[(q + 2) % 3] = u, v
    else:
        off[q], dc = j % 3 + 1, j // 3
    return off, dc


def slot_codes():
    codes = [0] * 128
    for kind, n in ((0, TURNS), (1, TURNS), (2, 6)):
        for j in range(n):
            for q in AXES:
                off, dc = offsets(kind, j, q)
                codes[54 * kind + 3 * j + q] = off[0] + 4 * off[1] + 16 * off[2] + 64 * dc
    codes[126] = 64
    assert sorted(codes) == list(range(128))
    return codes


def loop(lo, hi, fn):
    def body(i, carry):
        fn(i)
        return carry
    lax.fori_loop(lo, hi, body, 0)


def each(*fns):
    def body(j):
        for q in AXES:
            for fn in fns:
                fn(j, q)
    return body


def target(co, core, axis, off, dc):
    p = list(co)
    if axis is not None:
        p[axis] = (p[axis] + off) % 4
    return (0, (core + dc) % 2, p[2] * 16 + p[1] * 4 + p[0])


def iota(dim, *shape):
    return lax.broadcasted_iota(jnp.int32, shape, dim)


def onehot(mask, dtype=jnp.bfloat16):
    return jnp.where(mask, 1.0, 0.0).astype(dtype)


class Exchange:
    def __init__(self, co, core, sign, src, dst, rel, ssem, fsem, asem, rsem):
        self.co, self.core, self.sign = co, core, sign
        self.src, self.dst, self.rel = src, dst, rel
        self.ssem, self.fsem, self.asem, self.rsem = ssem, fsem, asem, rsem

    def to(self, axis, off, dc):
        return target(self.co, self.core, axis, self.sign * off + 4, dc)

    def copy(self, a, b, s, r, dest):
        return pltpu.make_async_remote_copy(a, b, s, r, device_id=dest, device_id_type=MESH)

    def a1(self, j, q):
        u, v, dc = dec(j)
        s = 3 * j + q
        self.copy(self.src.at[s], self.rel.at[s], self.ssem, self.asem.at[j], self.to(q, u, 0)).start()

    def a2(self, j, q):
        u, v, dc = dec(j)
        s = 3 * j + q
        self.copy(self.rel.at[s], self.rel.at[54 + s], self.fsem, self.asem.at[TURNS + j], self.to((q + 1) % 3, v, 0)).start()

    def a3(self, j, q):
        u, v, dc = dec(j)
        s = 3 * j + q
        self.copy(self.rel.at[54 + s], self.dst.at[s], self.fsem, self.rsem.at[(j + 10 - CUT) // 10], self.to((q + 2) % 3, third(q, u, v), dc)).start()

    def b1(self, j, q):
        u, v, dc = dec(j)
        s = 3 * j + q
        self.copy(self.src.at[54 + s], self.rel.at[108 + s], self.ssem, self.asem.at[2 * TURNS + j], self.to((q + 1) % 3, u, 0)).start()

    def b2(self, j, q):
        u, v, dc = dec(j)
        s = 3 * j + q
        self.copy(self.rel.at[108 + s], self.dst.at[54 + s], self.fsem, self.rsem.at[2 + (j + 10 - CUT) // 10], self.to((q + 2) % 3, v, dc)).start()

    def c1(self, k, q):
        s = 108 + 3 * k + q
        self.copy(self.src.at[s], self.dst.at[s], self.ssem, self.rsem.at[4], self.to(q, k % 3 + 1, k // 3)).start()

    def c0(self):
        self.copy(self.src.at[126], self.dst.at[126], self.ssem, self.rsem.at[4], self.to(None, 0, 1)).start()

    def wait(self, ref, sem):
        pltpu.make_async_remote_copy(ref, ref, self.ssem, sem, device_id=self.to(None, 0, 1), device_id_type=MESH).wait_recv()

    def wait_a1(self, j):
        self.wait(self.rel.at[pl.ds(3 * j, 3)], self.asem.at[j])

    def wait_a2(self, j):
        self.wait(self.rel.at[pl.ds(54 + 3 * j, 3)], self.asem.at[TURNS + j])

    def wait_b1(self, j):
        self.wait(self.rel.at[pl.ds(108 + 3 * j, 3)], self.asem.at[2 * TURNS + j])

    def wait_group(self, g):
        lo, n = GROUPS[g]
        n = n - 1 if g == 4 else n
        self.wait(self.dst.at[pl.ds(lo, n)], self.rsem.at[g])

    def drain(self):
        self.wait(self.src.at[pl.ds(0, 127)], self.ssem)
        self.wait(self.rel, self.fsem)


EARLY, LATE = 3 * CUT, 54 - 3 * CUT
GROUPS = ((0, EARLY), (EARLY, LATE), (54, EARLY), (54 + EARLY, LATE), (108, 20))


def kernel(code_hbm, idx_hbm, gates_hbm, tok_hbm, wg_hbm, wu_hbm, wd_hbm, out_ref,
           code_ref, idx_ref, gates_ref, tok_ref, wg, wu, wd, toka, idxa, bld, mid, rbuf, xg, ybuf, ret, rel2, rm_ref, gk_ref, acc, hbuf,
           *rest):
    gx_refs = rest[:5]
    wsem, ssem, tsem, isem, bsem, csem, asem2, rsem2 = rest[5:]
    c = lax.axis_index('ep2')
    e = lax.axis_index('ep')
    me = (e % 4, (e // 4) % 4, e // 16)
    bf = jnp.bfloat16
    f32 = jnp.float32

    cps = [pltpu.make_async_copy(wg_hbm, wg, wsem.at[0]), pltpu.make_async_copy(wu_hbm, wu, wsem.at[1]),
           pltpu.make_async_copy(wd_hbm, wd, wsem.at[2])]
    small = [pltpu.make_async_copy(a, b, wsem.at[3 + i]) for i, (a, b) in enumerate(
        ((idx_hbm, idx_ref), (tok_hbm, tok_ref), (gates_hbm, gates_ref), (code_hbm, code_ref)))]
    back = Exchange(me, c, -1, ybuf, ret, rel2, ssem.at[4], ssem.at[5], asem2, rsem2)

    def to(axis, off, dc):
        return target(me, c, axis, off, dc)

    for q in small:
        q.start()
    bar = pltpu.get_barrier_semaphore()

    def sig(k):
        for axis in AXES:
            for dc in range(2):
                pl.semaphore_signal(bar, inc=1, device_id=to(axis, k, dc), device_id_type=MESH)

    loop(1, 4, sig)
    pl.semaphore_signal(bar, inc=1, device_id=to(None, 0, 1), device_id_type=MESH)
    before = onehot(iota(0, T, T) < iota(1, T, T))

    def ranked(idx8, want):
        m = jnp.zeros(want.shape, f32)
        for j in range(8):
            m = jnp.where(idx8[j:j + 1, :] == want, 1.0, m)
        rank = jnp.dot(m.astype(bf), before, preferred_element_type=f32)
        return jnp.where(m > 0.5, rank + 1.0, 0.0)

    def select(idx8, p):
        k = iota(0, 32, 128)
        b, d = (p + 1) % 3, (p + 2) % 3
        want = (((c + (k >> 4)) & 1) * 64 + me[p] * WEIGHT[p] + ((me[b] + (k >> 2)) & 3) * WEIGHT[b]
                + ((me[d] + k) & 3) * WEIGHT[d])
        rm = ranked(idx8, want).astype(bf)
        ex = onehot((iota(0, 256, 32) >> 3) == iota(1, 256, 32))
        r = jnp.dot(ex, rm, preferred_element_type=f32)
        return onehot(r == ((iota(0, 256, T) & 7) + 1).astype(f32))

    def cols(p):
        return pl.ds(COLS[p][0], COLS[p][1])

    def build(p, a):
        n = COLS[p][1]
        if a == 0:
            rows = jnp.dot(select(idx_ref[...], p), tok_ref[:, cols(p)], preferred_element_type=f32).astype(bf)
        else:
            rows = jnp.dot(select(idxa[p, a - 1], p), toka[a - 1, :, cols(p)], preferred_element_type=f32).astype(bf)
        rows = rows.reshape(2, 4, 4, 8, n)
        for dc in range(2):
            mid[dc, 0, a, :, :, cols(p)] = rows[dc, 0]
            for v in NEXT:
                bld[dc, v - 1, a, :, :, cols(p)] = rows[dc, v]

    def remote(a, b, s, r, dest):
        return pltpu.make_async_remote_copy(a, b, s, r, device_id=dest, device_id_type=MESH)

    def take(ref, sem):
        remote(ref, ref, ssem.at[0], sem, to(None, 0, 1)).wait_recv()

    def gather_tokens():
        for u in (1, 3, 2):
            for p in AXES:
                remote(idx_ref, idxa.at[p, u - 1], ssem.at[0], isem.at[p, u - 1], to(p, u, 0)).start()
                if u != 2:
                    remote(tok_ref.at[:, cols(p)], toka.at[u - 1, :, cols(p)], ssem.at[1], tsem.at[p, u - 1], to(p, u, 0)).start()

    def pass_on(p, a):
        lo_c, n = COLS[p]
        part = pl.ds(lo_c, 384) if a == 1 else pl.ds(lo_c + 384, n - 384)
        remote(toka.at[a - 1, :, part], toka.at[1, :, part], ssem.at[6], tsem.at[p, 1], to(p, a, 0)).start()

    def second(dc, a, p):
        for v in NEXT:
            remote(bld.at[dc, v - 1, a, :, :, cols(p)], mid.at[dc, v, a, :, :, cols(p)], ssem.at[2], bsem.at[dc, p, v - 1],
                   to((p + 1) % 3, v, 0)).start()

    def place(p, v, w, dc, ref):
        if p == 0:
            return ref.at[dc, w, v, :, :, cols(0)]
        if p == 1:
            return ref.at[dc, v, :, w, :, cols(1)]
        return ref.at[dc, :, w, v, :, cols(2)]

    def last(dc, v):
        for p in AXES:
            if v:
                take(mid.at[dc, v, :, :, :, cols(p)], bsem.at[dc, p, v - 1])
            for w in range(1 - dc, 4):
                remote(mid.at[dc, v, :, w, :, cols(p)], place(p, v, w, dc, rbuf), ssem.at[3 + 4 * dc], csem.at[dc, p],
                       to((p + 2) % 3, w, dc) if w else to(None, 0, 1)).start()
            if dc == 0:
                place(p, v, 0, 0, rbuf)[...] = mid[0, v, :, 0, :, cols(p)]

    for q in small:
        q.wait()
    for p in AXES:
        build(p, 0)
    pl.semaphore_wait(bar, 19)
    for q in cps:
        q.start()
    gather_tokens()
    for p in AXES:
        second(0, 0, p)
    for a in (1, 3):
        for p in AXES:
            take(toka.at[a - 1, :, cols(p)], tsem.at[p, a - 1])
            pass_on(p, a)
    for a in NEXT:
        for p in AXES:
            take(idxa.at[p, a - 1], isem.at[p, a - 1])
            if a == 2:
                take(toka.at[a - 1, :, cols(p)], tsem.at[p, a - 1])
            build(p, a)
            second(0, a, p)
    last(0, 0)
    for a in (0, 1, 3):
        for p in AXES:
            second(1, a, p)

    rel = (((idx_ref[...] >> 6) - c) & 1) << 6
    for d in AXES:
        rel += (((idx_ref[...] >> (2 * d)) - me[d]) & 3) << (2 * d)
    want = code_ref[...]
    rm_ref[...] = jnp.swapaxes(ranked(rel, want), 0, 1).astype(bf)
    gk = jnp.zeros((T, T), f32)
    for j in range(8):
        gk = jnp.where(rel[j:j + 1, :] == want, gates_ref[j:j + 1, :], gk)
    gk = jnp.swapaxes(gk, 0, 1)
    hi = gk.astype(bf)
    r1 = gk - hi.astype(f32)
    md = r1.astype(bf)
    lo = (r1 - md.astype(f32)).astype(bf)
    gk_ref[...] = jnp.concatenate([hi, md, lo], axis=0)

    def spread(first, n):
        return onehot(iota(0, T, n) == first + (iota(1, T, n) >> 3))

    def chosen(n, ex):
        r = jnp.dot(rm_ref[...], ex, preferred_element_type=f32)
        return onehot(r == ((iota(1, T, n) & 7) + 1).astype(f32), f32)

    for g in range(5):
        ex = spread(GROUPS[g][0], GROUPS[g][1] * 8)
        on = chosen(GROUPS[g][1] * 8, ex)
        gx = jnp.dot(gk_ref[...], ex, preferred_element_type=f32)
        gx_refs[g][...] = (gx * jnp.concatenate([on, on, on], axis=0)).astype(bf)


    for v in NEXT:
        last(0, v)
    for p in AXES:
        second(1, 2, p)
    for v in (0, *NEXT):
        last(1, v)
    for q in cps:
        q.wait()

    def fetch(kind, lo_j, hi_j):
        def body(j):
            for q in AXES:
                off, dc = offsets(kind, j, q)
                xg[3 * (j - lo_j) + q] = rbuf[dc, off[2], off[1], off[0]]
        loop(lo_j, hi_j, body)

    def arrived(dc):
        if dc == 0:
            take(rbuf.at[0, 1:4, :, :, :, cols(0)], csem.at[0, 0])
            take(rbuf.at[0, :, :, 1:4, :, cols(1)], csem.at[0, 1])
            take(rbuf.at[0, :, 1:4, :, :, cols(2)], csem.at[0, 2])
        else:
            for p in AXES:
                take(rbuf.at[1, :, :, :, :, cols(p)], csem.at[1, p])

    def ffn(g):
        lo_s, n = GROUPS[g]
        rows = n * 8

        def up(f):
            fs = pl.ds(pl.multiple_of(f * 768, 768), 768)
            x = xg[0:n].reshape(rows, 2048)
            a = jnp.dot(x, wg[:, fs], preferred_element_type=f32)
            b = jnp.dot(x, wu[:, fs], preferred_element_type=f32)
            hbuf[0:rows, fs] = (a * jax.nn.sigmoid(a) * b).astype(bf)

        loop(0, 1, up)

        def down(t):
            ns = pl.ds(pl.multiple_of(t * 2048, 2048), 2048)
            y = jnp.dot(hbuf[0:rows, :], wd[:, ns], preferred_element_type=f32).astype(bf)
            ybuf[lo_s:lo_s + n, :, ns] = y.reshape(n, 8, 2048)

        loop(0, 1, down)

    def mix(g, first, last):
        lo_s, n = GROUPS[g]
        rows = n * 8
        gx = gx_refs[g][...]
        back.wait_group(g)

        def part(t):
            ns = pl.ds(pl.multiple_of(t * 2048, 2048), 2048)
            y = ret[lo_s:lo_s + n, :, ns].reshape(rows, 2048)
            p = jnp.dot(gx, y, preferred_element_type=f32)
            p = p[:T] + p[T:2 * T] + p[2 * T:]
            base = tok_ref[:, ns].astype(f32) if first else acc[:, ns]
            if last:
                out_ref[:, ns] = (base + p).astype(bf)
            else:
                acc[:, ns] = base + p

        loop(0, 1, part)

    def fwd(x, wait, move):
        def body(j):
            wait(j)
            for q in AXES:
                move(j, q)
        return body

    arrived(0)
    fetch(0, 0, CUT)
    ffn(0)
    loop(0, CUT, each(back.a1))
    fetch(1, 0, CUT)
    ffn(2)
    loop(0, CUT, each(back.b1))
    arrived(1)
    fetch(0, CUT, TURNS)
    ffn(1)
    loop(CUT, TURNS, each(back.a1))
    loop(0, CUT, fwd(back, back.wait_a1, back.a2))
    fetch(1, CUT, TURNS)
    ffn(3)
    loop(CUT, TURNS, each(back.b1))
    loop(CUT, TURNS, fwd(back, back.wait_a1, back.a2))
    fetch(2, 0, 6)
    for dc in range(2):
        xg[19 - dc] = rbuf[dc, 0, 0, 0]
    ffn(4)
    ret[127] = ybuf[127]
    back.c0()
    loop(0, 6, each(back.c1))
    loop(0, CUT, fwd(back, back.wait_a2, back.a3))
    loop(0, CUT, fwd(back, back.wait_b1, back.b2))
    loop(CUT, TURNS, fwd(back, back.wait_a2, back.a3))
    loop(CUT, TURNS, fwd(back, back.wait_b1, back.b2))
    take(idxa, ssem.at[0])
    take(toka.at[0:2], ssem.at[1])
    take(toka.at[0], ssem.at[6])
    take(bld, ssem.at[2])
    take(mid.at[0, :, :, 1:4], ssem.at[3])
    take(mid.at[1], ssem.at[7])
    mix(4, True, False)
    mix(0, False, False)
    mix(2, False, False)
    mix(1, False, False)
    mix(3, False, True)
    back.drain()


def solution(mesh):
    row_spec = P(('dp', 'ep2', 'ep'), None)
    weight_spec = P(('ep2', 'ep'), None, None)

    def local_step(tokens, expert_idx, gates, w_gate, w_up, w_down):
        vm = pl.BlockSpec(memory_space=pltpu.VMEM)
        anyw = pl.BlockSpec(memory_space=pl.ANY)
        bf = jnp.bfloat16
        codes = jnp.array(np.repeat(np.array(slot_codes(), np.int32)[:, None], 128, axis=1))
        dma = pltpu.SemaphoreType.DMA

        def vmem(*shape):
            return pltpu.VMEM(shape, bf)

        def rows(*shape):
            return vmem(*shape, 8, D)

        return pl.pallas_call(
            kernel,
            out_shape=jax.ShapeDtypeStruct((128, D), bf),
            in_specs=[anyw] * 7,
            out_specs=vm,
            scratch_shapes=[
                pltpu.VMEM((T, T), jnp.int32), pltpu.VMEM((8, T), jnp.int32), pltpu.VMEM((8, T), jnp.float32), vmem(T, D),
                vmem(D, 768), vmem(D, 768), vmem(768, D),
                vmem(3, T, D), pltpu.VMEM((3, 3, 8, T), jnp.int32),
                rows(2, 3, 4, 4), rows(*HALF), rows(*HALF), rows(32), rows(T), rows(T), rows(9 * TURNS),
                vmem(T, T), vmem(3 * T, T), pltpu.VMEM((T, D), jnp.float32), vmem(256, 768),
                *[vmem(3 * T, n * 8) for _, n in GROUPS],
                *[dma(n) for n in ((7,), (8,), (3, 3), (3, 3), (2, 3, 3), (2, 3), (3 * TURNS,), (5,))],
            ],
            compiler_params=pltpu.CompilerParams(collective_id=0, has_side_effects=True, vmem_limit_bytes=60 << 20),
        )(codes, expert_idx.T, gates.T, tokens, w_gate[0], w_up[0], w_down[0])

    return jax.shard_map(local_step, mesh=mesh, in_specs=(row_spec, row_spec, row_spec, weight_spec, weight_spec, weight_spec),
                         out_specs=row_spec, check_vma=False)
```

```python
import jax
import jax.numpy as jnp
from jax import lax
from jax.experimental import pallas as pl
from jax.experimental.pallas import tpu as pltpu
from jax.sharding import PartitionSpec as P

MESH = pl.DeviceIdType.MESH
D = 2048
T = 128
F = 768
AXES = range(3)
CORES = range(2)
NEXT = (1, 3, 2)
COLS = ((0, 768), (768, 640), (1408, 640))
SPLIT = 384
WEIGHT = (1, 4, 16)
CUBE = (2, 4, 4, 4)


def iota(dim, *shape):
    return lax.broadcasted_iota(jnp.int32, shape, dim)


def onehot(mask):
    return jnp.where(mask, 1.0, 0.0).astype(jnp.bfloat16)


def cols(p):
    return pl.ds(COLS[p][0], COLS[p][1])


def half(p, side):
    lo, n = COLS[p]
    return pl.ds(lo + SPLIT, n - SPLIT) if side else pl.ds(lo, SPLIT)


def place(p, v, w, dc, ref):
    if p == 0:
        return ref.at[dc, w, v, :, :, cols(0)]
    if p == 1:
        return ref.at[dc, v, :, w, :, cols(1)]
    return ref.at[dc, :, w, v, :, cols(2)]


def kernel(idx_hbm, gates_hbm, tok_hbm, wg_hbm, wu_hbm, wd_hbm, out_ref,
           idx_ref, gates_ref, tok_ref, wg, wu, wd, toka, idxa, gata, bld, mid, rbuf, ybuf, rmid, rbld,
           gxs, psum, phalf, pfin, acc, hbuf,
           wsem, ssem, isem, gsem, tsem, bsem, csem, cback, bback, hsem, fsem):
    c = lax.axis_index('ep2')
    e = lax.axis_index('ep')
    me = (e % 4, (e // 4) % 4, e // 16)
    bf = jnp.bfloat16
    f32 = jnp.float32

    def to(axis, off, dc):
        p = list(me)
        if axis is not None:
            p[axis] = (p[axis] + off) % 4
        return (0, (c + dc) % 2, p[2] * 16 + p[1] * 4 + p[0])

    small = [pltpu.make_async_copy(a, b, wsem.at[i]) for i, (a, b) in enumerate(
        ((idx_hbm, idx_ref), (tok_hbm, tok_ref), (gates_hbm, gates_ref)))]
    cps = [pltpu.make_async_copy(a, b, wsem.at[3 + i]) for i, (a, b) in enumerate(
        ((wg_hbm, wg), (wu_hbm, wu), (wd_hbm, wd)))]
    for q in small:
        q.start()
    bar = pltpu.get_barrier_semaphore()

    def sig(k, carry):
        for axis in AXES:
            for dc in CORES:
                pl.semaphore_signal(bar, inc=1, device_id=to(axis, k, dc), device_id_type=MESH)
        return carry

    lax.fori_loop(1, 4, sig, 0)
    pl.semaphore_signal(bar, inc=1, device_id=to(None, 0, 1), device_id_type=MESH)

    before = onehot(iota(0, T, T) < iota(1, T, T))
    widen = onehot((iota(0, 256, 32) >> 3) == iota(1, 256, 32))

    def select(idx8, g8, p, a):
        k = iota(0, 32, T)
        b, d = (p + 1) % 3, (p + 2) % 3
        want = (((c + (k >> 4)) & 1) * 64 + me[p] * WEIGHT[p] + ((me[b] + (k >> 2)) & 3) * WEIGHT[b]
                + ((me[d] + k) & 3) * WEIGHT[d])
        m = jnp.zeros(want.shape, f32)
        g = m
        for j in range(8):
            hit = idx8[j:j + 1, :] == want
            m = jnp.where(hit, 1.0, m)
            g = jnp.where(hit, g8[j:j + 1, :], g)
        rank = jnp.dot(m.astype(bf), before, preferred_element_type=f32)
        rm = jnp.where(m > 0.5, rank + 1.0, 0.0).astype(bf)
        r = jnp.dot(widen, rm, preferred_element_type=f32)
        on = r == ((iota(0, 256, T) & 7) + 1).astype(f32)
        hi = g.astype(bf)
        r1 = g - hi.astype(f32)
        md = r1.astype(bf)
        lo = (r1 - md.astype(f32)).astype(bf)
        for i, part in enumerate((hi, md, lo)):
            gx = jnp.where(on, jnp.dot(widen, part, preferred_element_type=f32), 0.0)
            gxs[p, a, i * T:i * T + T, :] = jnp.swapaxes(gx, 0, 1).astype(bf)
        return onehot(on)

    def build(p, a):
        n = COLS[p][1]
        if a == 0:
            sel, src = select(idx_ref[...], gates_ref[...], p, a), tok_ref[:, cols(p)]
        else:
            sel, src = select(idxa[p, a - 1], gata[p, a - 1], p, a), toka[a - 1, :, cols(p)]
        rows = jnp.dot(sel, src, preferred_element_type=f32).astype(bf).reshape(2, 4, 4, 8, n)
        for dc in CORES:
            mid[dc, 0, a, :, :, cols(p)] = rows[dc, 0]
            for v in NEXT:
                bld[dc, v - 1, a, :, :, cols(p)] = rows[dc, v]

    def send(a, b, s, r, dest):
        pltpu.make_async_remote_copy(a, b, ssem.at[s], r, device_id=dest, device_id_type=MESH).start()

    def take(ref, sem):
        pltpu.make_async_remote_copy(ref, ref, ssem.at[0], sem, device_id=to(None, 0, 1), device_id_type=MESH).wait_recv()

    def gather_tokens():
        for u in NEXT:
            for p in AXES:
                send(idx_ref, idxa.at[p, u - 1], 0, isem.at[u - 1], to(p, u, 0))
                if u != 2:
                    send(tok_ref.at[:, cols(p)], toka.at[u - 1, :, cols(p)], 1, tsem.at[p, u - 1], to(p, u, 0))
                send(gates_ref, gata.at[p, u - 1], 2, gsem.at[u - 1], to(p, u, 0))

    def second(dc, a):
        for p in AXES:
            for v in NEXT:
                send(bld.at[dc, v - 1, a, :, :, cols(p)], mid.at[dc, v, a, :, :, cols(p)], 3, bsem.at[dc, p, v - 1],
                     to((p + 1) % 3, v, 0))

    def last(dc, v):
        for p in AXES:
            if v:
                take(mid.at[dc, v, :, :, :, cols(p)], bsem.at[dc, p, v - 1])
            for w in range(1 - dc, 4):
                send(mid.at[dc, v, :, w, :, cols(p)], place(p, v, w, dc, rbuf), 4 + dc, csem.at[dc, p],
                     to((p + 2) % 3 if w else None, w, dc))
            if dc == 0:
                place(p, v, 0, 0, rbuf)[...] = mid[0, v, :, 0, :, cols(p)]

    for q in small:
        q.wait()
    for p in AXES:
        build(p, 0)
    pl.semaphore_wait(bar, 19)
    for q in cps:
        q.start()
    gather_tokens()
    second(0, 0)
    for a in (1, 3):
        for p in AXES:
            take(toka.at[a - 1, :, cols(p)], tsem.at[p, a - 1])
            send(toka.at[a - 1, :, half(p, a // 2)], toka.at[1, :, half(p, a // 2)], 6, tsem.at[p, 1], to(p, a, 0))
    for a in NEXT:
        take(idxa.at[:, a - 1], isem.at[a - 1])
        take(gata.at[:, a - 1], gsem.at[a - 1])
        for p in AXES:
            if a == 2:
                take(toka.at[1, :, cols(p)], tsem.at[p, 1])
            build(p, a)
        second(0, a)
    last(0, 0)
    for a in (0, 1, 3):
        second(1, a)
    for v in NEXT:
        last(0, v)
    second(1, 2)
    for v in (0, *NEXT):
        last(1, v)
    for q in cps:
        q.wait()

    def ffn(dc, h):
        x = rbuf[dc, 2 * h:2 * h + 2].reshape(256, D)
        a = jnp.dot(x, wg[...], preferred_element_type=f32)
        b = jnp.dot(x, wu[...], preferred_element_type=f32)
        hbuf[...] = (a * jax.nn.sigmoid(a) * b).astype(bf)
        y = jnp.dot(hbuf[...], wd[...], preferred_element_type=f32).astype(bf)
        ybuf[dc, 2 * h:2 * h + 2] = y.reshape(2, 4, 4, 8, D)

    def first_back(dc, h):
        for v in (*NEXT, 0):
            for p in AXES:
                if p == 1 and v // 2 != h:
                    continue
                for w in range(4):
                    if p == 0 and w // 2 != h:
                        continue
                    part = pl.ds(2 * h, 2) if p == 2 else pl.ds(0, 4)
                    src = ybuf.at[dc, part, w, v, :, cols(p)] if p == 2 else place(p, v, w, dc, ybuf)
                    dst = rmid.at[dc, v, part, w, :, cols(p)]
                    if w or dc:
                        send(src, dst, 7 + dc, cback.at[dc, v, p], to((p + 2) % 3 if w else None, 4 - w, dc))
                    else:
                        dst[...] = src[...]

    def landed(dc, v):
        for p in AXES:
            take(rmid.at[dc, v, :, pl.ds(1 - dc, 3 + dc), :, cols(p)], cback.at[dc, v, p])

    def second_back(dc, v, a):
        for p in AXES:
            send(rmid.at[dc, v, a, :, :, cols(p)], rbld.at[dc, v, a, :, :, cols(p)], 9, bback.at[a, p],
                 to((p + 1) % 3, 4 - v, 0))

    def mix(p, a):
        take(rbld.at[:, pl.ds(1, 3), a, :, :, cols(p)], bback.at[a, p])
        y = rbld[:, :, a, :, :, cols(p)].reshape(256, COLS[p][1])
        s = jnp.dot(gxs[p, a], y, preferred_element_type=f32)
        return s[:T] + s[T:2 * T] + s[2 * T:]

    take(rbuf.at[0, 1:4, :, :, :, cols(0)], csem.at[0, 0])
    take(rbuf.at[0, :, :, 1:4, :, cols(1)], csem.at[0, 1])
    take(rbuf.at[0, :, 1:4, :, :, cols(2)], csem.at[0, 2])
    ffn(0, 0)
    first_back(0, 0)
    ffn(0, 1)
    first_back(0, 1)
    for p in AXES:
        take(rbuf.at[1, :, :, :, :, cols(p)], csem.at[1, p])
    ffn(1, 0)
    first_back(1, 0)
    ffn(1, 1)
    first_back(1, 1)
    for v in NEXT:
        landed(0, v)
        second_back(0, v, 2)
    for a in (1, 3):
        for v in NEXT:
            second_back(0, v, a)
    for v in NEXT:
        landed(1, v)
        second_back(1, v, 2)
    for a in (1, 3):
        for v in NEXT:
            second_back(1, v, a)
    for dc in CORES:
        for v in NEXT:
            second_back(dc, v, 0)
    landed(0, 0)
    landed(1, 0)
    for dc in CORES:
        rbld[dc, 0] = rmid[dc, 0]

    for p in AXES:
        psum[1, :, cols(p)] = mix(p, 2)
    for p in AXES:
        for side in CORES:
            send(psum.at[1, :, half(p, side)], phalf.at[:, half(p, side)], 10, hsem.at[p, side], to(p, 1 if side else 3, 0))
    def total(p, side, part):
        a = 2 * side + 1
        send(psum.at[a - 1, :, half(p, part)], pfin.at[side, :, half(p, part)], 11, fsem.at[side, p], to(p, 4 - a, 0))

    for side in CORES:
        for p in AXES:
            psum[2 * side, :, cols(p)] = mix(p, 2 * side + 1)
        for p in AXES:
            total(p, side, 1 - side)
    for side in CORES:
        for p in AXES:
            take(phalf.at[:, half(p, side)], hsem.at[p, side])
            psum[2 * side, :, half(p, side)] += phalf[:, half(p, side)]
        for p in AXES:
            total(p, side, side)
    for p in AXES:
        acc[:, cols(p)] = tok_ref[:, cols(p)].astype(f32) + mix(p, 0)
    for side in CORES:
        for p in AXES:
            take(pfin.at[side, :, cols(p)], fsem.at[side, p])
            if side:
                out_ref[:, cols(p)] = (acc[:, cols(p)] + pfin[side, :, cols(p)]).astype(bf)
            else:
                acc[:, cols(p)] += pfin[side, :, cols(p)]

    for i, ref in enumerate((idxa, toka.at[0:2], gata, bld, mid.at[0, :, :, 1:4], mid.at[1], toka.at[0],
                             rmid.at[0, :, :, 1:4], rmid.at[1], rbld.at[:, 1:4], phalf, pfin)):
        take(ref, ssem.at[i])


def solution(mesh):
    row_spec = P(('dp', 'ep2', 'ep'), None)
    weight_spec = P(('ep2', 'ep'), None, None)

    def local_step(tokens, expert_idx, gates, w_gate, w_up, w_down):
        bf, i32, f32 = jnp.bfloat16, jnp.int32, jnp.float32
        dma = pltpu.SemaphoreType.DMA

        def vmem(*shape, dtype=bf):
            return pltpu.VMEM(shape, dtype)

        def rows(*shape):
            return vmem(*shape, 8, D)

        return pl.pallas_call(
            kernel,
            out_shape=jax.ShapeDtypeStruct((T, D), bf),
            in_specs=[pl.BlockSpec(memory_space=pl.ANY)] * 6,
            out_specs=pl.BlockSpec(memory_space=pltpu.VMEM),
            scratch_shapes=[
                vmem(8, T, dtype=i32), vmem(8, T, dtype=f32), vmem(T, D), vmem(D, F), vmem(D, F), vmem(F, D),
                vmem(3, T, D), vmem(3, 3, 8, T, dtype=i32), vmem(3, 3, 8, T, dtype=f32), rows(2, 3, 4, 4),
                *[rows(*CUBE) for _ in range(5)],
                vmem(3, 4, 3 * T, 256), vmem(3, T, D, dtype=f32), vmem(T, D, dtype=f32), vmem(2, T, D, dtype=f32),
                vmem(T, D, dtype=f32), vmem(256, F),
                *[dma(n) for n in ((6,), (12,), (3,), (3,), (3, 3), (2, 3, 3), (2, 3), (2, 4, 3), (4, 3), (3, 2), (2, 3))],
            ],
            compiler_params=pltpu.CompilerParams(collective_id=0, has_side_effects=True, vmem_limit_bytes=62 << 20),
        )(expert_idx.T, gates.T, tokens, w_gate[0], w_up[0], w_down[0])

    return jax.shard_map(local_step, mesh=mesh, in_specs=(row_spec, row_spec, row_spec, weight_spec, weight_spec, weight_spec),
                         out_specs=row_spec, check_vma=False)
```

```python
import jax
import jax.numpy as jnp
from jax import lax
from jax.experimental import pallas as pl
from jax.experimental.pallas import tpu as pltpu
from jax.sharding import PartitionSpec as P

MESH = pl.DeviceIdType.MESH
D = 2048
T = 128
F = 768
AXES = range(3)
CORES = range(2)
NEXT = (1, 3, 2)
COLS = ((0, 640), (640, 640), (1280, 768))
SPLIT = 384
WEIGHT = (1, 4, 16)
CUBE = (2, 4, 4, 4)


def iota(dim, *shape):
    return lax.broadcasted_iota(jnp.int32, shape, dim)


def onehot(mask):
    return jnp.where(mask, 1.0, 0.0).astype(jnp.bfloat16)


def cols(p):
    return pl.ds(COLS[p][0], COLS[p][1])


def half(p, side):
    lo, n = COLS[p]
    return pl.ds(lo + SPLIT, n - SPLIT) if side else pl.ds(lo, SPLIT)


def place(p, v, w, dc, ref):
    if p == 0:
        return ref.at[dc, w, v, :, :, cols(0)]
    if p == 1:
        return ref.at[dc, v, :, w, :, cols(1)]
    return ref.at[dc, :, w, v, :, cols(2)]


def kernel(idx_hbm, gates_hbm, tok_hbm, wg_hbm, wu_hbm, wd_hbm, out_ref,
           idx_ref, gates_ref, tok_ref, wg, wu, wd, toka, idxa, gata, bld, mid, rbuf, ybuf, rmid, rbld,
           gxs, psum, phalf, pfin, acc, hbuf,
           wsem, ssem, isem, gsem, tsem, bsem, csem, cback, bback, hsem, fsem):
    c = lax.axis_index('ep2')
    e = lax.axis_index('ep')
    me = (e % 4, (e // 4) % 4, e // 16)
    bf = jnp.bfloat16
    f32 = jnp.float32

    def to(axis, off, dc):
        p = list(me)
        if axis is not None:
            p[axis] = (p[axis] + off) % 4
        return (0, (c + dc) % 2, p[2] * 16 + p[1] * 4 + p[0])

    small = [pltpu.make_async_copy(a, b, wsem.at[i]) for i, (a, b) in enumerate(
        ((idx_hbm, idx_ref), (tok_hbm, tok_ref), (gates_hbm, gates_ref)))]
    cps = [pltpu.make_async_copy(a, b, wsem.at[3 + i]) for i, (a, b) in enumerate(
        ((wg_hbm, wg), (wu_hbm, wu), (wd_hbm, wd)))]
    for q in small:
        q.start()
    bar = pltpu.get_barrier_semaphore()

    def sig(k, carry):
        for axis in AXES:
            for dc in CORES:
                pl.semaphore_signal(bar, inc=1, device_id=to(axis, k, dc), device_id_type=MESH)
        return carry

    lax.fori_loop(1, 4, sig, 0)
    pl.semaphore_signal(bar, inc=1, device_id=to(None, 0, 1), device_id_type=MESH)

    before = onehot(iota(0, T, T) < iota(1, T, T))
    widen = onehot((iota(0, 256, 32) >> 3) == iota(1, 256, 32))

    def select(idx8, g8, p, a):
        k = iota(0, 32, T)
        b, d = (p + 1) % 3, (p + 2) % 3
        want = (((c + (k >> 4)) & 1) * 64 + me[p] * WEIGHT[p] + ((me[b] + (k >> 2)) & 3) * WEIGHT[b]
                + ((me[d] + k) & 3) * WEIGHT[d])
        m = jnp.zeros(want.shape, f32)
        g = m
        for j in range(8):
            hit = idx8[j:j + 1, :] == want
            m = jnp.where(hit, 1.0, m)
            g = jnp.where(hit, g8[j:j + 1, :], g)
        rank = jnp.dot(m.astype(bf), before, preferred_element_type=f32)
        rm = jnp.where(m > 0.5, rank + 1.0, 0.0).astype(bf)
        r = jnp.dot(widen, rm, preferred_element_type=f32)
        on = r == ((iota(0, 256, T) & 7) + 1).astype(f32)
        hi = g.astype(bf)
        r1 = g - hi.astype(f32)
        md = r1.astype(bf)
        lo = (r1 - md.astype(f32)).astype(bf)
        for i, part in enumerate((hi, md, lo)):
            gx = jnp.where(on, jnp.dot(widen, part, preferred_element_type=f32), 0.0)
            gxs[p, a, i * T:i * T + T, :] = jnp.swapaxes(gx, 0, 1).astype(bf)
        return onehot(on)

    def build(p, a):
        n = COLS[p][1]
        if a == 0:
            sel, src = select(idx_ref[...], gates_ref[...], p, a), tok_ref[:, cols(p)]
        else:
            sel, src = select(idxa[p, a - 1], gata[p, a - 1], p, a), toka[a - 1, :, cols(p)]
        rows = jnp.dot(sel, src, preferred_element_type=f32).astype(bf).reshape(2, 4, 4, 8, n)
        for dc in CORES:
            mid[dc, 0, a, :, :, cols(p)] = rows[dc, 0]
            for v in NEXT:
                bld[dc, v - 1, a, :, :, cols(p)] = rows[dc, v]

    def send(a, b, s, r, dest):
        pltpu.make_async_remote_copy(a, b, ssem.at[s], r, device_id=dest, device_id_type=MESH).start()

    def take(ref, sem):
        pltpu.make_async_remote_copy(ref, ref, ssem.at[0], sem, device_id=to(None, 0, 1), device_id_type=MESH).wait_recv()

    def gather_tokens():
        for u in NEXT:
            for p in AXES:
                send(idx_ref, idxa.at[p, u - 1], 0, isem.at[u - 1], to(p, u, 0))
                if u != 2:
                    send(tok_ref.at[:, cols(p)], toka.at[u - 1, :, cols(p)], 1, tsem.at[p, u - 1], to(p, u, 0))
                send(gates_ref, gata.at[p, u - 1], 2, gsem.at[u - 1], to(p, u, 0))

    def second(dc, a):
        for p in AXES:
            for v in NEXT:
                send(bld.at[dc, v - 1, a, :, :, cols(p)], mid.at[dc, v, a, :, :, cols(p)], 3, bsem.at[dc, p, v - 1],
                     to((p + 1) % 3, v, 0))

    def last(dc, v):
        for p in AXES:
            if v:
                take(mid.at[dc, v, :, :, :, cols(p)], bsem.at[dc, p, v - 1])
            for w in range(1 - dc, 4):
                send(mid.at[dc, v, :, w, :, cols(p)], place(p, v, w, dc, rbuf), 4 + dc, csem.at[dc, p],
                     to((p + 2) % 3 if w else None, w, dc))
            if dc == 0:
                place(p, v, 0, 0, rbuf)[...] = mid[0, v, :, 0, :, cols(p)]

    for q in small:
        q.wait()
    for p in AXES:
        build(p, 0)
    pl.semaphore_wait(bar, 19)
    for q in cps:
        q.start()
    gather_tokens()
    second(0, 0)
    second(1, 0)
    for a in (1, 3):
        for p in AXES:
            take(toka.at[a - 1, :, cols(p)], tsem.at[p, a - 1])
            send(toka.at[a - 1, :, half(p, a // 2)], toka.at[1, :, half(p, a // 2)], 6, tsem.at[p, 1], to(p, a, 0))
    for a in NEXT:
        take(idxa.at[:, a - 1], isem.at[a - 1])
        take(gata.at[:, a - 1], gsem.at[a - 1])
        for p in AXES:
            if a == 2:
                take(toka.at[1, :, cols(p)], tsem.at[p, 1])
            build(p, a)
        second(0, a)
    last(0, 0)
    for a in (1, 3):
        second(1, a)
    for v in NEXT:
        last(0, v)
    second(1, 2)
    for v in (0, *NEXT):
        last(1, v)
    for q in cps:
        q.wait()

    def ffn(dc, h):
        x = rbuf[dc, 2 * h:2 * h + 2].reshape(256, D)
        a = jnp.dot(x, wg[...], preferred_element_type=f32)
        b = jnp.dot(x, wu[...], preferred_element_type=f32)
        hbuf[...] = (a * jax.nn.sigmoid(a) * b).astype(bf)
        y = jnp.dot(hbuf[...], wd[...], preferred_element_type=f32).astype(bf)
        ybuf[dc, 2 * h:2 * h + 2] = y.reshape(2, 4, 4, 8, D)

    def first_back(dc, h):
        for v in (*NEXT, 0):
            for p in AXES:
                if p == 1 and v // 2 != h:
                    continue
                for w in range(4):
                    if p == 0 and w // 2 != h:
                        continue
                    part = pl.ds(2 * h, 2) if p == 2 else pl.ds(0, 4)
                    src = ybuf.at[dc, part, w, v, :, cols(p)] if p == 2 else place(p, v, w, dc, ybuf)
                    dst = rmid.at[dc, v, part, w, :, cols(p)]
                    if w or dc:
                        send(src, dst, 7 + dc, cback.at[dc, v, p], to((p + 2) % 3 if w else None, 4 - w, dc))
                    else:
                        dst[...] = src[...]

    def landed(dc, v):
        for p in AXES:
            take(rmid.at[dc, v, :, pl.ds(1 - dc, 3 + dc), :, cols(p)], cback.at[dc, v, p])

    def second_back(dc, v, a):
        for p in AXES:
            send(rmid.at[dc, v, a, :, :, cols(p)], rbld.at[dc, v, a, :, :, cols(p)], 9, bback.at[a, p],
                 to((p + 1) % 3, 4 - v, 0))

    def mix(p, a):
        take(rbld.at[:, pl.ds(1, 3), a, :, :, cols(p)], bback.at[a, p])
        y = rbld[:, :, a, :, :, cols(p)].reshape(256, COLS[p][1])
        s = jnp.dot(gxs[p, a], y, preferred_element_type=f32)
        return s[:T] + s[T:2 * T] + s[2 * T:]

    take(rbuf.at[0, 1:4, :, :, :, cols(0)], csem.at[0, 0])
    take(rbuf.at[0, :, :, 1:4, :, cols(1)], csem.at[0, 1])
    take(rbuf.at[0, :, 1:4, :, :, cols(2)], csem.at[0, 2])
    ffn(0, 0)
    ffn(0, 1)
    first_back(0, 0)
    first_back(0, 1)
    for p in AXES:
        take(rbuf.at[1, :, :, :, :, cols(p)], csem.at[1, p])
    ffn(1, 0)
    first_back(1, 0)
    ffn(1, 1)
    first_back(1, 1)
    for v in NEXT:
        landed(0, v)
        second_back(0, v, 2)
    for a in (1, 3):
        for v in NEXT:
            second_back(0, v, a)
    for v in NEXT:
        landed(1, v)
        second_back(1, v, 2)
    for a in (1, 3):
        for v in NEXT:
            second_back(1, v, a)
    for dc in CORES:
        for v in NEXT:
            second_back(dc, v, 0)
    landed(0, 0)
    landed(1, 0)
    for dc in CORES:
        rbld[dc, 0] = rmid[dc, 0]

    for p in AXES:
        psum[1, :, cols(p)] = mix(p, 2)
    for p in AXES:
        for side in CORES:
            send(psum.at[1, :, half(p, side)], phalf.at[:, half(p, side)], 10, hsem.at[p, side], to(p, 1 if side else 3, 0))
    def total(p, side, part):
        a = 2 * side + 1
        send(psum.at[a - 1, :, half(p, part)], pfin.at[side, :, half(p, part)], 11, fsem.at[side, p], to(p, 4 - a, 0))

    for side in CORES:
        for p in AXES:
            psum[2 * side, :, cols(p)] = mix(p, 2 * side + 1)
        for p in AXES:
            total(p, side, 1 - side)
    for side in CORES:
        for p in AXES:
            take(phalf.at[:, half(p, side)], hsem.at[p, side])
            psum[2 * side, :, half(p, side)] += phalf[:, half(p, side)]
        for p in AXES:
            total(p, side, side)
    for p in AXES:
        acc[:, cols(p)] = tok_ref[:, cols(p)].astype(f32) + mix(p, 0)
    for side in CORES:
        for p in AXES:
            take(pfin.at[side, :, cols(p)], fsem.at[side, p])
            if side:
                out_ref[:, cols(p)] = (acc[:, cols(p)] + pfin[side, :, cols(p)]).astype(bf)
            else:
                acc[:, cols(p)] += pfin[side, :, cols(p)]

    for i, ref in enumerate((idxa, toka.at[0:2], gata, bld, mid.at[0, :, :, 1:4], mid.at[1], toka.at[0],
                             rmid.at[0, :, :, 1:4], rmid.at[1], rbld.at[:, 1:4], phalf, pfin)):
        take(ref, ssem.at[i])


def solution(mesh):
    row_spec = P(('dp', 'ep2', 'ep'), None)
    weight_spec = P(('ep2', 'ep'), None, None)

    def local_step(tokens, expert_idx, gates, w_gate, w_up, w_down):
        bf, i32, f32 = jnp.bfloat16, jnp.int32, jnp.float32
        dma = pltpu.SemaphoreType.DMA

        def vmem(*shape, dtype=bf):
            return pltpu.VMEM(shape, dtype)

        def rows(*shape):
            return vmem(*shape, 8, D)

        return pl.pallas_call(
            kernel,
            out_shape=jax.ShapeDtypeStruct((T, D), bf),
            in_specs=[pl.BlockSpec(memory_space=pl.ANY)] * 6,
            out_specs=pl.BlockSpec(memory_space=pltpu.VMEM),
            scratch_shapes=[
                vmem(8, T, dtype=i32), vmem(8, T, dtype=f32), vmem(T, D), vmem(D, F), vmem(D, F), vmem(F, D),
                vmem(3, T, D), vmem(3, 3, 8, T, dtype=i32), vmem(3, 3, 8, T, dtype=f32), rows(2, 3, 4, 4),
                *[rows(*CUBE) for _ in range(5)],
                vmem(3, 4, 3 * T, 256), vmem(3, T, D, dtype=f32), vmem(T, D, dtype=f32), vmem(2, T, D, dtype=f32),
                vmem(T, D, dtype=f32), vmem(256, F),
                *[dma(n) for n in ((6,), (12,), (3,), (3,), (3, 3), (2, 3, 3), (2, 3), (2, 4, 3), (4, 3), (3, 2), (2, 3))],
            ],
            compiler_params=pltpu.CompilerParams(collective_id=0, has_side_effects=True, vmem_limit_bytes=62 << 20),
        )(expert_idx.T, gates.T, tokens, w_gate[0], w_up[0], w_down[0])

    return jax.shard_map(local_step, mesh=mesh, in_specs=(row_spec, row_spec, row_spec, weight_spec, weight_spec, weight_spec),
                         out_specs=row_spec, check_vma=False)
```

```python
import jax
import jax.numpy as jnp
from jax import lax
from jax.experimental import pallas as pl
from jax.experimental.pallas import tpu as pltpu
from jax.sharding import PartitionSpec as P

MESH = pl.DeviceIdType.MESH
D = 2048
T = 128
F = 768
AXES = range(3)
CORES = range(2)
NEXT = (1, 3, 2)
COLS = ((0, 640), (640, 640), (1280, 768))
SPLIT = 384
WEIGHT = (1, 4, 16)
CUBE = (2, 4, 4, 4)


def iota(dim, *shape):
    return lax.broadcasted_iota(jnp.int32, shape, dim)


def onehot(mask):
    return jnp.where(mask, 1.0, 0.0).astype(jnp.bfloat16)


def cols(p):
    return pl.ds(COLS[p][0], COLS[p][1])


def half(p, side):
    lo, n = COLS[p]
    return pl.ds(lo + SPLIT, n - SPLIT) if side else pl.ds(lo, SPLIT)


def place(p, v, w, dc, ref):
    if p == 0:
        return ref.at[dc, w, v, :, :, cols(0)]
    if p == 1:
        return ref.at[dc, v, :, w, :, cols(1)]
    return ref.at[dc, :, w, v, :, cols(2)]


def kernel(idx_hbm, gates_hbm, tok_hbm, wg_hbm, wu_hbm, wd_hbm, out_ref,
           idx_ref, gates_ref, tok_ref, wg, wu, wd, toka, idxa, gata, bld, mid, rbuf, ybuf, rmid, rbld,
           gxs, psum, phalf, pfin, acc, hbuf,
           wsem, ssem, isem, gsem, tsem, bsem, csem, cback, bback, hsem, fsem):
    c = lax.axis_index('ep2')
    e = lax.axis_index('ep')
    me = (e % 4, (e // 4) % 4, e // 16)
    bf = jnp.bfloat16
    f32 = jnp.float32

    def to(axis, off, dc):
        p = list(me)
        if axis is not None:
            p[axis] = (p[axis] + off) % 4
        return (0, (c + dc) % 2, p[2] * 16 + p[1] * 4 + p[0])

    small = [pltpu.make_async_copy(a, b, wsem.at[i]) for i, (a, b) in enumerate(
        ((idx_hbm, idx_ref), (tok_hbm, tok_ref), (gates_hbm, gates_ref)))]
    cps = [pltpu.make_async_copy(a, b, wsem.at[3 + i]) for i, (a, b) in enumerate(
        ((wg_hbm, wg), (wu_hbm, wu), (wd_hbm, wd)))]
    for q in small:
        q.start()
    bar = pltpu.get_barrier_semaphore()

    def sig(k, carry):
        for axis in AXES:
            for dc in CORES:
                pl.semaphore_signal(bar, inc=1, device_id=to(axis, k, dc), device_id_type=MESH)
        return carry

    lax.fori_loop(1, 4, sig, 0)
    pl.semaphore_signal(bar, inc=1, device_id=to(None, 0, 1), device_id_type=MESH)

    before = onehot(iota(0, T, T) < iota(1, T, T))
    widen = onehot((iota(0, 256, 32) >> 3) == iota(1, 256, 32))

    def select(idx8, g8, p, a):
        k = iota(0, 32, T)
        b, d = (p + 1) % 3, (p + 2) % 3
        want = (((c + (k >> 4)) & 1) * 64 + me[p] * WEIGHT[p] + ((me[b] + (k >> 2)) & 3) * WEIGHT[b]
                + ((me[d] + k) & 3) * WEIGHT[d])
        m = jnp.zeros(want.shape, f32)
        g = m
        for j in range(8):
            hit = idx8[j:j + 1, :] == want
            m = jnp.where(hit, 1.0, m)
            g = jnp.where(hit, g8[j:j + 1, :], g)
        rank = jnp.dot(m.astype(bf), before, preferred_element_type=f32)
        rm = jnp.where(m > 0.5, rank + 1.0, 0.0).astype(bf)
        r = jnp.dot(widen, rm, preferred_element_type=f32)
        on = r == ((iota(0, 256, T) & 7) + 1).astype(f32)
        hi = g.astype(bf)
        r1 = g - hi.astype(f32)
        md = r1.astype(bf)
        lo = (r1 - md.astype(f32)).astype(bf)
        for i, part in enumerate((hi, md, lo)):
            gx = jnp.where(on, jnp.dot(widen, part, preferred_element_type=f32), 0.0)
            gxs[p, a, i * T:i * T + T, :] = jnp.swapaxes(gx, 0, 1).astype(bf)
        return onehot(on)

    def build(p, a):
        n = COLS[p][1]
        if a == 0:
            sel, src = select(idx_ref[...], gates_ref[...], p, a), tok_ref[:, cols(p)]
        else:
            sel, src = select(idxa[p, a - 1], gata[p, a - 1], p, a), toka[a - 1, :, cols(p)]
        rows = jnp.dot(sel, src, preferred_element_type=f32).astype(bf).reshape(2, 4, 4, 8, n)
        for dc in CORES:
            mid[dc, 0, a, :, :, cols(p)] = rows[dc, 0]
            for v in NEXT:
                bld[dc, v - 1, a, :, :, cols(p)] = rows[dc, v]

    def send(a, b, s, r, dest):
        pltpu.make_async_remote_copy(a, b, ssem.at[s], r, device_id=dest, device_id_type=MESH).start()

    def take(ref, sem):
        pltpu.make_async_remote_copy(ref, ref, ssem.at[0], sem, device_id=to(None, 0, 1), device_id_type=MESH).wait_recv()

    def gather_tokens():
        for u in NEXT:
            for p in AXES:
                send(idx_ref, idxa.at[p, u - 1], 0, isem.at[u - 1], to(p, u, 0))
                if u != 2:
                    send(tok_ref.at[:, cols(p)], toka.at[u - 1, :, cols(p)], 1, tsem.at[p, u - 1], to(p, u, 0))
                send(gates_ref, gata.at[p, u - 1], 2, gsem.at[u - 1], to(p, u, 0))

    def second(dc, a):
        for p in AXES:
            for v in NEXT:
                send(bld.at[dc, v - 1, a, :, :, cols(p)], mid.at[dc, v, a, :, :, cols(p)], 3, bsem.at[dc, p, v - 1],
                     to((p + 1) % 3, v, 0))

    def last(dc, v):
        for p in AXES:
            if v:
                take(mid.at[dc, v, :, :, :, cols(p)], bsem.at[dc, p, v - 1])
            for w in range(1 - dc, 4):
                send(mid.at[dc, v, :, w, :, cols(p)], place(p, v, w, dc, rbuf), 4 + dc, csem.at[dc, p],
                     to((p + 2) % 3 if w else None, w, dc))
            if dc == 0:
                place(p, v, 0, 0, rbuf)[...] = mid[0, v, :, 0, :, cols(p)]

    for q in small:
        q.wait()
    for p in AXES:
        build(p, 0)
    pl.semaphore_wait(bar, 19)
    for q in cps:
        q.start()
    gather_tokens()
    second(0, 0)
    second(1, 0)
    for a in (1, 3):
        for p in AXES:
            take(toka.at[a - 1, :, cols(p)], tsem.at[p, a - 1])
            send(toka.at[a - 1, :, half(p, a // 2)], toka.at[1, :, half(p, a // 2)], 6, tsem.at[p, 1], to(p, a, 0))
    for a in NEXT:
        take(idxa.at[:, a - 1], isem.at[a - 1])
        take(gata.at[:, a - 1], gsem.at[a - 1])
        for p in AXES:
            if a == 2:
                take(toka.at[1, :, cols(p)], tsem.at[p, 1])
            build(p, a)
        second(0, a)
    last(0, 0)
    for a in (1, 3):
        second(1, a)
    for v in NEXT:
        last(0, v)
    second(1, 2)
    for v in (0, *NEXT):
        last(1, v)
    for q in cps:
        q.wait()

    def ffn(dc, h):
        x = rbuf[dc, 2 * h:2 * h + 2].reshape(256, D)
        a = jnp.dot(x, wg[...], preferred_element_type=f32)
        b = jnp.dot(x, wu[...], preferred_element_type=f32)
        hbuf[...] = (a * jax.nn.sigmoid(a) * b).astype(bf)
        y = jnp.dot(hbuf[...], wd[...], preferred_element_type=f32).astype(bf)
        ybuf[dc, 2 * h:2 * h + 2] = y.reshape(2, 4, 4, 8, D)

    def first_back(dc, h):
        for v in (*NEXT, 0):
            for p in AXES:
                if p == 1 and v // 2 != h:
                    continue
                for w in range(4):
                    if p == 0 and w // 2 != h:
                        continue
                    part = pl.ds(2 * h, 2) if p == 2 else pl.ds(0, 4)
                    src = ybuf.at[dc, part, w, v, :, cols(p)] if p == 2 else place(p, v, w, dc, ybuf)
                    dst = rmid.at[dc, v, part, w, :, cols(p)]
                    if w or dc:
                        send(src, dst, 7 + dc, cback.at[dc, v], to((p + 2) % 3 if w else None, 4 - w, dc))
                    else:
                        dst[...] = src[...]

    def landed(dc, v):
        take(rmid.at[dc, v, :, pl.ds(1 - dc, 3 + dc)], cback.at[dc, v])

    def second_back(dc, v, a):
        for p in AXES:
            send(rmid.at[dc, v, a, :, :, cols(p)], rbld.at[dc, v, a, :, :, cols(p)], 9, bback.at[a],
                 to((p + 1) % 3, 4 - v, 0))

    def mix(p, a):
        if p == 0:
            take(rbld.at[:, pl.ds(1, 3), a], bback.at[a])
        y = rbld[:, :, a, :, :, cols(p)].reshape(256, COLS[p][1])
        s = jnp.dot(gxs[p, a], y, preferred_element_type=f32)
        return s[:T] + s[T:2 * T] + s[2 * T:]

    take(rbuf.at[0, 1:4, :, :, :, cols(0)], csem.at[0, 0])
    take(rbuf.at[0, :, :, 1:4, :, cols(1)], csem.at[0, 1])
    take(rbuf.at[0, :, 1:4, :, :, cols(2)], csem.at[0, 2])
    ffn(0, 0)
    ffn(0, 1)
    first_back(0, 0)
    first_back(0, 1)
    for p in AXES:
        take(rbuf.at[1, :, :, :, :, cols(p)], csem.at[1, p])
    ffn(1, 0)
    first_back(1, 0)
    ffn(1, 1)
    first_back(1, 1)
    for v in NEXT:
        landed(0, v)
        second_back(0, v, 2)
    for a in (1, 3):
        for v in NEXT:
            second_back(0, v, a)
    for v in NEXT:
        landed(1, v)
        second_back(1, v, 2)
    for a in (1, 3):
        for v in NEXT:
            second_back(1, v, a)
    for dc in CORES:
        for v in NEXT:
            second_back(dc, v, 0)
    landed(0, 0)
    landed(1, 0)
    for dc in CORES:
        rbld[dc, 0] = rmid[dc, 0]

    for p in AXES:
        psum[1, :, cols(p)] = mix(p, 2)
    for p in AXES:
        for side in CORES:
            send(psum.at[1, :, half(p, side)], phalf.at[:, half(p, side)], 10, hsem.at[p, side], to(p, 1 if side else 3, 0))
    def total(p, side, part):
        a = 2 * side + 1
        send(psum.at[a - 1, :, half(p, part)], pfin.at[side, :, half(p, part)], 11, fsem.at[side, p], to(p, 4 - a, 0))

    for side in CORES:
        for p in AXES:
            psum[2 * side, :, cols(p)] = mix(p, 2 * side + 1)
        for p in AXES:
            total(p, side, 1 - side)
    for side in CORES:
        for p in AXES:
            take(phalf.at[:, half(p, side)], hsem.at[p, side])
            psum[2 * side, :, half(p, side)] += phalf[:, half(p, side)]
        for p in AXES:
            total(p, side, side)
    for p in AXES:
        acc[:, cols(p)] = tok_ref[:, cols(p)].astype(f32) + mix(p, 0)
    for side in CORES:
        for p in AXES:
            take(pfin.at[side, :, cols(p)], fsem.at[side, p])
            if side:
                out_ref[:, cols(p)] = (acc[:, cols(p)] + pfin[side, :, cols(p)]).astype(bf)
            else:
                acc[:, cols(p)] += pfin[side, :, cols(p)]

    for i, ref in enumerate((idxa, toka.at[0:2], gata, bld, mid.at[0, :, :, 1:4], mid.at[1], toka.at[0],
                             rmid.at[0, :, :, 1:4], rmid.at[1], rbld.at[:, 1:4], phalf, pfin)):
        take(ref, ssem.at[i])


def solution(mesh):
    row_spec = P(('dp', 'ep2', 'ep'), None)
    weight_spec = P(('ep2', 'ep'), None, None)

    def local_step(tokens, expert_idx, gates, w_gate, w_up, w_down):
        bf, i32, f32 = jnp.bfloat16, jnp.int32, jnp.float32
        dma = pltpu.SemaphoreType.DMA

        def vmem(*shape, dtype=bf):
            return pltpu.VMEM(shape, dtype)

        def rows(*shape):
            return vmem(*shape, 8, D)

        return pl.pallas_call(
            kernel,
            out_shape=jax.ShapeDtypeStruct((T, D), bf),
            in_specs=[pl.BlockSpec(memory_space=pl.ANY)] * 6,
            out_specs=pl.BlockSpec(memory_space=pltpu.VMEM),
            scratch_shapes=[
                vmem(8, T, dtype=i32), vmem(8, T, dtype=f32), vmem(T, D), vmem(D, F), vmem(D, F), vmem(F, D),
                vmem(3, T, D), vmem(3, 3, 8, T, dtype=i32), vmem(3, 3, 8, T, dtype=f32), rows(2, 3, 4, 4),
                *[rows(*CUBE) for _ in range(5)],
                vmem(3, 4, 3 * T, 256), vmem(3, T, D, dtype=f32), vmem(T, D, dtype=f32), vmem(2, T, D, dtype=f32),
                vmem(T, D, dtype=f32), vmem(256, F),
                *[dma(n) for n in ((6,), (12,), (3,), (3,), (3, 3), (2, 3, 3), (2, 3), (2, 4), (4,), (3, 2), (2, 3))],
            ],
            compiler_params=pltpu.CompilerParams(collective_id=0, has_side_effects=True, vmem_limit_bytes=62 << 20),
        )(expert_idx.T, gates.T, tokens, w_gate[0], w_up[0], w_down[0])

    return jax.shard_map(local_step, mesh=mesh, in_specs=(row_spec, row_spec, row_spec, weight_spec, weight_spec, weight_spec),
                         out_specs=row_spec, check_vma=False)
```
